256 devices in a mesh: sub: 64 (over x, z, core), tile: 4 (over y).
Axes of the slice: x: 4, y: 4, z: 8, core: 2. Of those that a mesh axis runs over, the one named last changes fastest.
Arguments:
- coupling: bfloat16 [64, 28, 256, 256], P('sub'), may hold values from -0.125 to 0.125
- panel_inv: float32 [64, 8, 256, 256], P('sub')
- a_ib: bfloat16 [64, 2048, 3072], P('sub', None, 'tile'), may hold values from -0.5 to 0.5
- owner: int32 [64, 12, 12], P('sub', None, 'tile'), may hold values from 0 to 63, as said below
- slot: int32 [64, 12, 12], P('sub', None, 'tile'), may hold values from 0 to 15
- base: bfloat16 [64, 64, 256, 256], P('sub', 'tile'), may hold values from -2 to 2
Outputs:
- assembled: bfloat16 [64, 64, 256, 256], P('sub', 'tile')
The draws below stay inside these ranges and needn't reach their ends.
Inputs may be any that keep to these rules, and one draw needn't show every extreme that they name: `owner`: tiles of one device are those of one subdomain s and tile columns t*12/4 to (t+1)*12/4 - 1. At most 1 tiles of one device name one sub index; for each t one sub index, drawn from the seed, is named by exactly 1 tiles of every device of that t.
All inputs are finite; a program needn't handle non-finite values.
Results may differ from the reference program's by a relative error of at most 0.0051.
Values may be sent and summed in bfloat16 or wider, within the bound.
A program may use at most 128 MiB of HBM per device.

```python
import math
import jax
import jax.numpy as jnp
from jax import lax

NI = 2048
NB = 3072
PANEL = 256
SLOTS = 16
LOWER = 28
NBT = 12
SUBS = 64
OWNED = 64
N_SUB = 64
N_TILE = 4


def draw_panel_inv(key, part):
    random_key = jax.random.fold_in(key, 1)
    shape = (SUBS, NI // PANEL, PANEL, PANEL)
    random_part = jax.random.normal(random_key, shape, jnp.float32)
    identity = jnp.eye(PANEL, dtype=jnp.float32)
    return 0.6 * identity + 0.3 * random_part / math.sqrt(PANEL)


def draw_owner(key, part):
    tile_side = NB // PANEL
    tile_count = tile_side * tile_side // N_TILE
    capacity = (tile_count + N_SUB - 1) // N_SUB
    others = (N_SUB - 1) * capacity
    hot_key, seat_key = jax.random.split(key)
    hottest = jax.random.randint(hot_key, (N_TILE,), 0, N_SUB).astype(jnp.int32)

    def one_device(device_key, hot_owner):
        first_key, second_key = jax.random.split(device_key)
        seat_order = jax.random.permutation(first_key, others)[:tile_count - capacity].astype(jnp.int32)
        chosen = (hot_owner + 1 + seat_order // capacity) % N_SUB
        listed = jnp.concatenate([jnp.full((capacity,), hot_owner, jnp.int32), chosen.astype(jnp.int32)])
        return listed[jax.random.permutation(second_key, tile_count)]
    device_keys = jax.random.split(seat_key, SUBS * N_TILE)
    hot_all = jnp.tile(hottest, SUBS)
    drawn = jax.vmap(one_device)(device_keys, hot_all)
    drawn = drawn.reshape(SUBS, N_TILE, tile_side, tile_count // tile_side)
    return drawn.transpose(0, 2, 1, 3).reshape(SUBS, tile_side, tile_side)


def set_ends(array, rng, least, high):
    extent = array.shape
    index_at = [jax.random.randint(jax.random.fold_in(rng, axis), (), 0, extent[axis]) for axis in range(len(extent))]
    array = array.at[tuple(index_at)].set(least)
    longest = extent.index(max(extent))
    index_at[longest] = (index_at[longest] + 1) % extent[longest]
    return array.at[tuple(index_at)].set(high)


def level_of(stream_key, dims, cuts, low, top_value):
    loudness, own = 1.0, jax.random.fold_in(stream_key, 6)
    for axis_at, parts in cuts:
        steps = jnp.exp(jax.random.uniform(jax.random.fold_in(own, axis_at), (parts,), jnp.float32, low / len(cuts), top_value / len(cuts)))
        loudness = loudness * jnp.repeat(steps, dims[axis_at] // parts).reshape([-1 if axis == axis_at else 1 for axis in range(len(dims))])
    return loudness


def scatter_about(key, shape, scale, most, pieces=(), kind=jnp.bfloat16):
    values = scale * jax.random.normal(key, shape, jnp.float32)
    if pieces:
        values = values * level_of(key, shape, pieces, -0.22, 0.18)
    return jnp.clip(values, -most, most).astype(kind)


def setup_inputs(seed: int = 0) -> dict:
    key_of = jax.random.split(jax.random.key(seed), 7)
    coupling = scatter_about(key_of[0], (SUBS, LOWER, PANEL, PANEL), NI ** -0.5, 0.125, ((0, 64),))
    panel_inv = draw_panel_inv(jax.random.fold_in(key_of[6], 71), 0)
    a_ib = scatter_about(key_of[2], (SUBS, NI, NB), 0.0625, 0.5, ((0, 64), (2, 4)))
    owner = draw_owner(jax.random.fold_in(key_of[6], 71), 0)
    slot = set_ends(jax.random.randint(key_of[4], (SUBS, NBT, NBT), 0, SLOTS), jax.random.fold_in(key_of[4], 1), 0, SLOTS - 1).astype(jnp.int32)
    base = scatter_about(key_of[5], (SUBS, OWNED, PANEL, PANEL), 0.3, 2.0, ((0, 64), (1, 4)))
    return dict(coupling=coupling, panel_inv=panel_inv, a_ib=a_ib, owner=owner, slot=slot, base=base)


def solve(lower_blocks, inverse, right_cols):
    panel_width = inverse.shape[1]
    panels = []
    for row_panel in range(inverse.shape[0]):
        target = right_cols[row_panel * panel_width:(row_panel + 1) * panel_width].astype(jnp.float32)
        if row_panel > 0:
            block_start = row_panel * (row_panel - 1) // 2
            blocks = lower_blocks[block_start:block_start + row_panel]
            joined = jnp.transpose(blocks, (1, 0, 2)).reshape(panel_width, row_panel * panel_width)
            target = target - jnp.dot(joined, jnp.concatenate(panels, axis=0), preferred_element_type=jnp.float32)
        solved_panel = jnp.dot(inverse[row_panel], target, precision=lax.Precision.HIGHEST, preferred_element_type=jnp.float32)
        panels.append(solved_panel.astype(jnp.bfloat16))
    return jnp.concatenate(panels, axis=0)


def reference(coupling, panel_inv, a_ib, owner, slot, base):
    tile_side = NB // PANEL
    col_tiles = tile_side // N_TILE
    column_group = jnp.arange(tile_side, dtype=jnp.int32) // col_tiles

    def assemble_one(accumulated, operands):
        lower_blocks, inverse, right_cols, owner_ids, slot_ids = operands
        solved = solve(lower_blocks, inverse, right_cols)
        gram_matrix = lax.dot_general(solved, solved, (((0,), (0,)), ((), ())), preferred_element_type=jnp.float32)
        contrib = (-gram_matrix).astype(jnp.bfloat16)
        contrib = lax.optimization_barrier(contrib).astype(jnp.float32)
        tiled = contrib.reshape(tile_side, PANEL, tile_side, PANEL).transpose(0, 2, 1, 3)
        places = column_group[None, :] * SLOTS + slot_ids
        accumulated = accumulated.at[owner_ids, places].add(tiled)
        return accumulated, None

    start_total = jnp.zeros((SUBS, OWNED, PANEL, PANEL), jnp.float32)
    accumulated, _ = lax.scan(assemble_one, start_total, (coupling, panel_inv, a_ib, owner, slot))
    return (base.astype(jnp.float32) + accumulated).astype(jnp.bfloat16)
```

```python
import functools

import jax
import jax.numpy as jnp
from jax import lax
from jax.experimental import pallas as pl
from jax.experimental.pallas import tpu as pltpu
from jax.sharding import PartitionSpec as P

MESH = pl.DeviceIdType.MESH
NX, NZ, NC, NY = 4, 8, 2, 4
PW = 256
NQ = 16
R = PW // NQ
VMEM_LIMIT = 67043328
NT = (((1,), (1,)), ((), ()))


def dot_nt(left, right):
    return lax.dot_general(left, right, NT, preferred_element_type=jnp.float32)


def split_hi_lo(value):
    high = value.astype(jnp.bfloat16)
    low = (value - high.astype(jnp.float32)).astype(jnp.bfloat16)
    return high, low


def solve_kernel(owner_s, slot_s, c_ref, inv_ref, a_ref, y_ref, idx_s, pages_ref, lab_s):
    t = lax.axis_index("tile")
    for j in range(64):
        idx_s[j] = 36
        lab_s[j] = -1
    for a in range(12):
        d = lax.rem(a // 3 - t + NY, NY)
        rel = jnp.where(d == 0, 0, jnp.where(d == 3, 1, jnp.where(d == 1, 2, 3)))
        for b in range(3):
            o = owner_s[a, b]
            seat = ((o // 16) * 2 + lax.rem(o, 2)) * 8 + lax.rem(o // 2, 8)
            idx_s[seat] = (rel * 3 + a % 3) * 3 + b
            lab_s[seat] = slot_s[a, b]
    for j in range(64):
        pages_ref[j // 8, j % 8] = jnp.full((8, 128), lab_s[j], jnp.int32)
    for k in range(8):
        target = a_ref[k * PW : (k + 1) * PW, :].astype(jnp.float32).T
        if k:
            start = k * (k - 1) // 2
            joined = jnp.concatenate([c_ref[start + m] for m in range(k)], axis=1)
            target = target - dot_nt(y_ref[:, : k * PW], joined)
        t_hi, t_lo = split_hi_lo(target)
        i_hi, i_lo = split_hi_lo(inv_ref[k])
        solved = dot_nt(
            jnp.concatenate([t_hi, t_hi, t_lo], axis=1), jnp.concatenate([i_hi, i_lo, i_hi], axis=1)
        )
        y_ref[:, k * PW : (k + 1) * PW] = solved.astype(jnp.bfloat16)


def combine(dense, tiles, write):
    for half in range(2):
        cols = slice(half * 128, half * 128 + 128)
        acc = [None] * 16
        for view in dense:
            for j in range(16):
                x = view(j, cols).astype(jnp.float32)
                acc[j] = x if acc[j] is None else acc[j] + x
        for view, page in tiles:
            x = view(cols).astype(jnp.float32)
            lab = page()
            lab = jnp.concatenate([lab] * (R // 8), axis=0)
            for j in range(16):
                term = jnp.where(lab == j, x, 0.0)
                acc[j] = term if acc[j] is None else acc[j] + term
        for j in range(16):
            write(j, cols, acc[j])


def exchange_kernel(
    idx_s, pages, own, base, out,
    G, S, RA, T, B1, B2, B3, B4, C3, C4, tiles, RL, L1, L2,
    sy, ry, sa, sf, ra, rt, sz, rz, sl, rl, rlz,
):
    s = lax.axis_index("sub")
    t = lax.axis_index("tile")
    x, z, c = s // 16, lax.rem(s // 2, NZ), lax.rem(s, 2)
    g_own = x * 2 + c

    def at(dx, dz, core, dt):
        xx = lax.rem(x + dx + NX, NX)
        zz = lax.rem(z + dz + NZ, NZ)
        return ((xx * NZ + zz) * NC + core, lax.rem(t + dt + NY, NY))

    def group(dx, core):
        return lax.rem(x + dx + NX, NX) * 2 + core

    def zat(dz):
        return lax.rem(z + dz + NZ, NZ)

    def rc(src, dst, ss, rs, dev):
        return pltpu.make_async_remote_copy(
            src_ref=src, dst_ref=dst, send_sem=ss, recv_sem=rs, device_id=dev, device_id_type=MESH
        )

    direct = [(1, 0), (1, 1), (-1, 0), (-1, 1), (0, 1 - c)]
    two = [(2, 0), (2, 1)]

    def y_direct(q, i):
        return rc(own.at[:, q], G.at[q, i], sy.at[q, i], ry.at[q, i], at(0, 0, c, (1, -1)[i]))

    def y_forward(q, i):
        lanes = pl.ds(i * 1024, 1024)
        return rc(
            G.at[q, i, :, :, lanes], G.at[q, 2, :, :, lanes],
            sy.at[q, 2 + i], ry.at[q, 2 + i], at(0, 0, c, (1, -1)[i]),
        )

    def a_direct(q, i):
        dx, core = direct[i]
        return rc(
            S.at[q, group(dx, core)], RA.at[q, :, g_own], sa.at[q, i], ra.at[q, g_own], at(dx, 0, core, 0)
        )

    def a_transit(q, i):
        return rc(
            S.at[q, group(2, i)], T.at[q, i], sa.at[q, 5 + i], rt.at[q, i], at((1, -1)[i], 0, c, 0)
        )

    def a_forward(q, i):
        src_g = group((-1, 1)[i], c)
        return rc(
            T.at[q, i], RA.at[q, :, src_g], sf.at[q, i], ra.at[q, src_g], at((1, -1)[i], 0, i, 0)
        )

    def a_arrival(q, g):
        return rc(S.at[q, g], RA.at[q, :, g], sa.at[q, 0], ra.at[q, g], at(0, 0, 1 - c, 0))

    def z_copy(q, d, h):
        sign = 1 - 2 * d
        dev = at(0, sign, c, 0)
        if h == 0:
            src, dst = RA.at[q, zat(4), pl.ds(4 * d, 4)], B1.at[d, q]
        elif h == 1:
            src, dst = B1.at[d, q], B2.at[d, q, pl.ds(0, 4)]
        elif h == 2:
            src, dst = RA.at[q, zat(3 * sign)], B2.at[d, q, pl.ds(4, 8)]
        elif h == 3:
            src, dst = C3.at[d, q], B3.at[d, q]
        else:
            src, dst = C4.at[d, q], B4.at[d, q]
        return rc(src, dst, sz.at[q, d * 5 + h], rz.at[q, d * 5 + h], dev)

    def label_group(i):
        dx, core = (direct + two)[i]
        return rc(pages.at[group(dx, core)], RL.at[:, g_own], sl.at[i], rl.at[g_own], at(dx, 0, core, 0))

    def label_arrival(g):
        return rc(pages.at[g], RL.at[:, g], sl.at[0], rl.at[g], at(0, 0, 1 - c, 0))

    def label_z(d, i):
        sign = 1 - 2 * d
        if i == 0:
            src, dst = RL.at[zat(3 * sign)], L1.at[d]
        else:
            src, dst = RL.at[zat(4), pl.ds(4 * d, 4)], L2.at[d]
        return rc(src, dst, sl.at[7 + 2 * d + i], rlz.at[2 * d + i], at(0, sign * (1 + i), c, 0))

    barrier = pltpu.get_barrier_semaphore()
    peers = [at(dx, 0, core, 0) for dx, core in direct + two]
    peers += [at(0, dz, c, 0) for dz in (1, -1, 2, -2)] + [at(0, 0, c, dt) for dt in (1, -1)]
    for dev in peers:
        pl.semaphore_signal(barrier, inc=1, device_id=dev, device_id_type=MESH)
    pl.semaphore_wait(barrier, len(peers))

    for i in range(2):
        y_direct(0, i).start()
    for i in range(7):
        label_group(i).start()
    tiles[36] = jnp.zeros((R, PW), jnp.bfloat16)
    for zz in range(NZ):
        RL[zz, g_own] = pages[g_own, zz]
    for i in range(1, 8):
        label_arrival(lax.rem(g_own + i, 8)).wait_recv()
    for d in range(2):
        for i in range(2):
            label_z(d, i).start()
    for i in range(2):
        y_direct(0, i).wait_recv()
        y_forward(0, i).start()
    for q in (1, 2):
        for i in range(2):
            y_direct(q, i).start()
    for d in range(2):
        for i in range(2):
            label_z(d, i).wait_recv()

    def tile_view(ref, *index):
        return lambda cols: ref[(*index, slice(None), cols)]

    def page_view(ref, *index):
        return lambda: ref[index]

    def tick(step, carry):
        def stage(lag, run):
            q = step - lag

            @pl.when(jnp.logical_and(q >= 0, q < NQ))
            def _():
                run(q)

        def finish(q):
            for d in range(2):
                z_copy(q, d, 4).wait_recv()
            rows = pl.ds(pl.multiple_of(q * R, R), R)

            def write(j, cols, value):
                out[j, rows, cols] = value.astype(jnp.bfloat16)

            combine(
                [lambda j, cols: base[j, rows, cols]]
                + [lambda j, cols, d=d: B4[d, q, j, :, cols] for d in range(2)],
                [(tile_view(RA, q, z, g), page_view(RL, z, g)) for g in range(8)],
                write,
            )

        def hop4(q):
            for d in range(2):
                sign = 1 - 2 * d
                z_copy(q, d, 3).wait_recv()

                def write(j, cols, value, d=d):
                    C4[d, q, j, :, cols] = value.astype(jnp.bfloat16)

                combine(
                    [lambda j, cols, d=d: B3[d, q, j, :, cols]],
                    [(tile_view(RA, q, zat(sign), g), page_view(RL, zat(sign), g)) for g in range(8)],
                    write,
                )
                z_copy(q, d, 4).start()

        def hop3(q):
            for d in range(2):
                sign = 1 - 2 * d
                z_copy(q, d, 1).wait_recv()
                z_copy(q, d, 2).wait_recv()

                def write(j, cols, value, d=d):
                    C3[d, q, j, :, cols] = value.astype(jnp.bfloat16)

                combine(
                    [],
                    [(tile_view(B2, d, q, i), page_view(L2, d, i)) for i in range(4)]
                    + [(tile_view(B2, d, q, 4 + i), page_view(L1, d, i)) for i in range(8)]
                    + [(tile_view(RA, q, zat(2 * sign), g), page_view(RL, zat(2 * sign), g)) for g in range(8)],
                    write,
                )
                z_copy(q, d, 3).start()

        def hop2(q):
            for d in range(2):
                z_copy(q, d, 0).wait_recv()
                z_copy(q, d, 1).start()
                z_copy(q, d, 2).start()

        def hop1(q):
            for i in range(1, 8):
                a_arrival(q, lax.rem(g_own + i, 8)).wait_recv()
            for d in range(2):
                z_copy(q, d, 0).start()

        def relay(q):
            for i in range(2):
                a_transit(q, i).wait_recv()
                a_forward(q, i).start()

        def form(q):
            for i in range(2):
                y_forward(q, i).wait_recv()
            left = jnp.concatenate(
                [own[:, q].reshape(3 * R, 2048), G[q].reshape(9 * R, 2048)], axis=0
            )
            for b in range(3):
                gram = dot_nt(left, own[b].reshape(PW, 2048))
                for p in range(12):
                    tiles[p * 3 + b] = (-gram[p * R : (p + 1) * R]).astype(jnp.bfloat16)
            for j in range(64):
                S[q, j // 8, j % 8] = tiles[idx_s[j]]
            for i in range(2):
                a_transit(q, i).start()
            for i in range(5):
                a_direct(q, i).start()
            for zz in range(NZ):
                RA[q, zz, g_own] = S[q, g_own, zz]

        def gather(q):
            for i in range(2):
                y_direct(q, i).wait_recv()
                y_forward(q, i).start()

        def lead(q):
            for i in range(2):
                y_direct(q, i).start()

        stage(6, finish)
        stage(5, hop4)
        stage(4, hop3)
        stage(3, hop2)
        stage(2, hop1)
        stage(1, relay)
        stage(0, form)

        @pl.when(step + 1 < NQ)
        def _():
            gather(step + 1)

        @pl.when(step + 3 < NQ)
        def _():
            lead(step + 3)

        return carry

    lax.fori_loop(0, NQ + 6, tick, 0)

    def drain(q, carry):
        for i in range(2):
            y_direct(q, i).wait_send()
            y_forward(q, i).wait_send()
            a_transit(q, i).wait_send()
            a_forward(q, i).wait_send()
        for i in range(5):
            a_direct(q, i).wait_send()
        for d in range(2):
            for h in range(5):
                z_copy(q, d, h).wait_send()
        return carry

    lax.fori_loop(0, NQ, drain, 0)
    for i in range(7):
        label_group(i).wait_send()
    for d in range(2):
        for i in range(2):
            label_z(d, i).wait_send()


def shards(coupling, panel_inv, a_ib, owner, slot, base):
    vmem = pl.BlockSpec(memory_space=pltpu.VMEM)
    smem = pl.BlockSpec(memory_space=pltpu.SMEM)
    bf16, i32 = jnp.bfloat16, jnp.int32
    solved, idx, pages = pl.pallas_call(
        solve_kernel,
        out_shape=(
            jax.ShapeDtypeStruct((768, 2048), bf16),
            jax.ShapeDtypeStruct((64,), i32),
            jax.ShapeDtypeStruct((8, 8, 8, 128), i32),
        ),
        in_specs=[smem, smem, vmem, vmem, vmem],
        out_specs=(vmem, smem, vmem),
        scratch_shapes=[pltpu.SMEM((64,), i32)],
        compiler_params=pltpu.CompilerParams(vmem_limit_bytes=VMEM_LIMIT),
        name="solve",
    )(owner[0], slot[0], coupling[0], panel_inv[0], a_ib[0])
    dma = pltpu.SemaphoreType.DMA
    result = pl.pallas_call(
        exchange_kernel,
        out_shape=jax.ShapeDtypeStruct((16, PW, PW), bf16),
        in_specs=[smem, vmem, vmem, vmem],
        out_specs=vmem,
        scratch_shapes=[
            pltpu.VMEM((NQ, 3, 3, R, 2048), bf16),
            pltpu.VMEM((NQ, 8, 8, R, PW), bf16),
            pltpu.VMEM((NQ, 8, 8, R, PW), bf16),
            pltpu.VMEM((NQ, 2, 8, R, PW), bf16),
            pltpu.VMEM((2, NQ, 4, R, PW), bf16),
            pltpu.VMEM((2, NQ, 12, R, PW), bf16),
            pltpu.VMEM((2, NQ, 16, R, PW), bf16),
            pltpu.VMEM((2, NQ, 16, R, PW), bf16),
            pltpu.VMEM((2, NQ, 16, R, PW), bf16),
            pltpu.VMEM((2, NQ, 16, R, PW), bf16),
            pltpu.VMEM((37, R, PW), bf16),
            pltpu.VMEM((8, 8, 8, 128), i32),
            pltpu.VMEM((2, 8, 8, 128), i32),
            pltpu.VMEM((2, 4, 8, 128), i32),
            dma((NQ, 4)), dma((NQ, 4)),
            dma((NQ, 7)), dma((NQ, 2)), dma((NQ, 8)), dma((NQ, 2)),
            dma((NQ, 10)), dma((NQ, 10)),
            dma((11,)), dma((8,)), dma((4,)),
        ],
        compiler_params=pltpu.CompilerParams(
            collective_id=0, has_side_effects=True, vmem_limit_bytes=VMEM_LIMIT
        ),
        name="exchange",
    )(idx, pages, solved.reshape(3, NQ, R, 2048), base[0])
    return result[None]


def solution(mesh):
    placed = (
        P("sub", None, None, None),
        P("sub", None, None, None),
        P("sub", None, "tile"),
        P("sub", None, "tile"),
        P("sub", None, "tile"),
        P("sub", "tile", None, None),
    )
    return jax.shard_map(
        shards, mesh=mesh, in_specs=placed, out_specs=P("sub", "tile", None, None), check_vma=False
    )
```

```python
import functools

import jax
import jax.numpy as jnp
from jax import lax
from jax.experimental import pallas as pl
from jax.experimental.pallas import tpu as pltpu
from jax.sharding import PartitionSpec as P

MESH = pl.DeviceIdType.MESH
NX, NZ, NC, NY = 4, 8, 2, 4
PW = 256
NQ = 16
R = PW // NQ
FIRST = 4
RING = 4
VMEM_LIMIT = 67043328
NT = (((1,), (1,)), ((), ()))


def dot_nt(left, right):
    return lax.dot_general(left, right, NT, preferred_element_type=jnp.float32)


def split_hi_lo(value):
    high = value.astype(jnp.bfloat16)
    low = (value - high.astype(jnp.float32)).astype(jnp.bfloat16)
    return high, low


def combine(dense, tiles, write):
    for half in range(2):
        cols = slice(half * 128, half * 128 + 128)
        acc = [None] * 16
        for view in dense:
            for j in range(16):
                x = view(j, cols).astype(jnp.float32)
                acc[j] = x if acc[j] is None else acc[j] + x
        for view, page in tiles:
            x = view(cols).astype(jnp.float32)
            lab = page()
            lab = jnp.concatenate([lab] * (R // 8), axis=0)
            for j in range(16):
                term = jnp.where(lab == j, x, 0.0)
                acc[j] = term if acc[j] is None else acc[j] + term
        for j in range(16):
            write(j, cols, acc[j])


def schur_kernel(
    owner_s, slot_s, c_hbm, inv_hbm, a_hbm, base_hbm, out,
    c_v, inv_v, a_v, base, own, seats_v, seats_s, pages,
    G, S, RA, T, B1, B2, B3, B4, C3, C4, tiles, RL, L1, L2,
    ld, sy, ry, sa, sf, ra, rt, sz, rz, sl, rl, rlz,
):
    s = lax.axis_index("sub")
    t = lax.axis_index("tile")
    x, z, c = s // 16, lax.rem(s // 2, NZ), lax.rem(s, 2)
    g_own = x * 2 + c

    def at(dx, dz, core, dt):
        xx = lax.rem(x + dx + NX, NX)
        zz = lax.rem(z + dz + NZ, NZ)
        return ((xx * NZ + zz) * NC + core, lax.rem(t + dt + NY, NY))

    def group(dx, core):
        return lax.rem(x + dx + NX, NX) * 2 + core

    def zat(dz):
        return lax.rem(z + dz + NZ, NZ)

    def rc(src, dst, ss, rs, dev):
        return pltpu.make_async_remote_copy(
            src_ref=src, dst_ref=dst, send_sem=ss, recv_sem=rs, device_id=dev, device_id_type=MESH
        )

    direct = [(1, 0), (1, 1), (-1, 0), (-1, 1), (0, 1 - c)]
    two = [(2, 0), (2, 1)]

    def y_direct(q, i):
        return rc(own.at[:, q], G.at[q, i], sy.at[q, i], ry.at[q, i], at(0, 0, c, (1, -1)[i]))

    def y_forward(q, i):
        lanes = pl.ds(i * 1024, 1024)
        return rc(
            G.at[q, i, :, :, lanes], G.at[q, 2, :, :, lanes],
            sy.at[q, 2 + i], ry.at[q, 2 + i], at(0, 0, c, (1, -1)[i]),
        )

    def a_direct(q, i):
        dx, core = direct[i]
        return rc(
            S.at[q, group(dx, core)], RA.at[q, :, g_own], sa.at[q, i], ra.at[q, g_own], at(dx, 0, core, 0)
        )

    def a_transit(q, i):
        return rc(
            S.at[q, group(2, i)], T.at[q, i], sa.at[q, 5 + i], rt.at[q, i], at((1, -1)[i], 0, c, 0)
        )

    def a_forward(q, i):
        src_g = group((-1, 1)[i], c)
        return rc(
            T.at[q, i], RA.at[q, :, src_g], sf.at[q, i], ra.at[q, src_g], at((1, -1)[i], 0, i, 0)
        )

    def a_arrival(q, g):
        return rc(S.at[q, g], RA.at[q, :, g], sa.at[q, 0], ra.at[q, g], at(0, 0, 1 - c, 0))

    def z_copy(q, d, h):
        sign = 1 - 2 * d
        dev = at(0, sign, c, 0)
        if h == 0:
            src, dst = RA.at[q, zat(4), pl.ds(4 * d, 4)], B1.at[d, q]
        elif h == 1:
            src, dst = B1.at[d, q], B2.at[d, q, pl.ds(0, 4)]
        elif h == 2:
            src, dst = RA.at[q, zat(3 * sign)], B2.at[d, q, pl.ds(4, 8)]
        elif h == 3:
            src, dst = C3.at[d, lax.rem(q, RING)], B3.at[d, q]
        else:
            src, dst = C4.at[d, lax.rem(q, RING)], B4.at[d, q]
        return rc(src, dst, sz.at[q, d * 5 + h], rz.at[q, d * 5 + h], dev)

    def label_group(i):
        dx, core = (direct + two)[i]
        return rc(pages.at[group(dx, core)], RL.at[:, g_own], sl.at[i], rl.at[g_own], at(dx, 0, core, 0))

    def label_arrival(g):
        return rc(pages.at[g], RL.at[:, g], sl.at[0], rl.at[g], at(0, 0, 1 - c, 0))

    def label_z(d, i):
        sign = 1 - 2 * d
        if i == 0:
            src, dst = RL.at[zat(3 * sign)], L1.at[d]
        else:
            src, dst = RL.at[zat(4), pl.ds(4 * d, 4)], L2.at[d]
        return rc(src, dst, sl.at[7 + 2 * d + i], rlz.at[2 * d + i], at(0, sign * (1 + i), c, 0))

    def loads(k):
        rows = pl.ds(k * PW, PW)
        copies = [
            pltpu.make_async_copy(a_hbm.at[rows], a_v.at[rows], ld.at[k, 0]),
            pltpu.make_async_copy(inv_hbm.at[k], inv_v.at[k], ld.at[k, 1]),
        ]
        if k:
            blocks = pl.ds(k * (k - 1) // 2, k)
            copies.append(pltpu.make_async_copy(c_hbm.at[blocks], c_v.at[blocks], ld.at[k, 2]))
        return copies

    def solve_panel(k, first, last):
        count = 3 * (last - first) * R
        cols = slice(k * PW, (k + 1) * PW)
        target = own[:, first:last, :, cols].reshape(count, PW).astype(jnp.float32)
        if k:
            start = k * (k - 1) // 2
            joined = jnp.concatenate([c_v[start + m] for m in range(k)], axis=1)
            target = target - dot_nt(own[:, first:last, :, : k * PW].reshape(count, k * PW), joined)
        t_hi, t_lo = split_hi_lo(target)
        i_hi, i_lo = split_hi_lo(inv_v[k])
        solved = dot_nt(
            jnp.concatenate([t_hi, t_hi, t_lo], axis=1), jnp.concatenate([i_hi, i_lo, i_hi], axis=1)
        )
        own[:, first:last, :, cols] = solved.astype(jnp.bfloat16).reshape(3, last - first, R, PW)

    def gather_chunk(q):
        for i in range(2):
            y_direct(q, i).wait_recv()
            y_forward(q, i).start()

    for k in range(8):
        for copy in loads(k):
            copy.start()
    base_load = pltpu.make_async_copy(base_hbm, base, ld.at[8, 0])
    base_load.start()

    barrier = pltpu.get_barrier_semaphore()
    peers = [at(dx, 0, core, 0) for dx, core in direct + two]
    peers += [at(0, dz, c, 0) for dz in (1, -1, 2, -2)] + [at(0, 0, c, dt) for dt in (1, -1)]
    for dev in peers:
        pl.semaphore_signal(barrier, inc=1, device_id=dev, device_id_type=MESH)

    for k in range(8):
        for copy in loads(k):
            copy.wait()
        cols = slice(k * PW, (k + 1) * PW)
        rows = a_v[cols, :].T
        own[:, :, :, cols] = rows.reshape(3, NQ, R, PW)
        solve_panel(k, 0, FIRST)
    pl.semaphore_wait(barrier, len(peers))
    for i in range(2):
        y_direct(0, i).start()

    lane = lax.broadcasted_iota(jnp.int32, (8, 128), 1)
    seat_tile = jnp.full((8, 128), 36, jnp.int32)
    seat_slot = jnp.full((8, 128), -1, jnp.int32)
    for a in range(12):
        d = lax.rem(a // 3 - t + NY, NY)
        rel = jnp.where(d == 0, 0, jnp.where(d == 3, 1, jnp.where(d == 1, 2, 3)))
        for b in range(3):
            o = owner_s[b, 0, a]
            seat = ((o // 16) * 2 + lax.rem(o, 2)) * 8 + lax.rem(o // 2, 8)
            here = lane == seat
            seat_tile = jnp.where(here, (rel * 3 + a % 3) * 3 + b, seat_tile)
            seat_slot = jnp.where(here, slot_s[b, 0, a], seat_slot)
    seats_v[0] = seat_tile
    seats_v[1] = seat_slot
    to_scalar = pltpu.make_async_copy(seats_v, seats_s, ld.at[8, 1])
    to_scalar.start()
    to_scalar.wait()
    for j in range(64):
        pages[j // 8, j % 8] = jnp.full((8, 128), seats_s[1, 0, j], jnp.int32)
    for i in range(7):
        label_group(i).start()
    for k in range(8):
        solve_panel(k, FIRST, NQ)
        if k == 5:
            gather_chunk(0)
            for q in (1, 2):
                for i in range(2):
                    y_direct(q, i).start()
    tiles[36] = jnp.zeros((R, PW), jnp.bfloat16)
    for zz in range(NZ):
        RL[zz, g_own] = pages[g_own, zz]
    base_load.wait()

    def tile_view(ref, *index):
        return lambda cols: ref[(*index, slice(None), cols)]

    def page_view(ref, *index):
        return lambda: ref[index]

    def tick(step, carry):
        def stage(lag, run):
            q = step - lag

            @pl.when(jnp.logical_and(q >= 0, q < NQ))
            def _():
                run(q)

        def finish(q):
            for d in range(2):
                z_copy(q, d, 4).wait_recv()
            rows = pl.ds(pl.multiple_of(q * R, R), R)

            def write(j, cols, value):
                out[j, rows, cols] = value.astype(jnp.bfloat16)

            combine(
                [lambda j, cols: base[j, rows, cols]]
                + [lambda j, cols, d=d: B4[d, q, j, :, cols] for d in range(2)],
                [(tile_view(RA, q, z, g), page_view(RL, z, g)) for g in range(8)],
                write,
            )

        def hop4(q):
            for d in range(2):
                sign = 1 - 2 * d
                z_copy(q, d, 3).wait_recv()

                @pl.when(q >= RING)
                def _(d=d):
                    z_copy(q - RING, d, 4).wait_send()

                def write(j, cols, value, d=d):
                    C4[d, lax.rem(q, RING), j, :, cols] = value.astype(jnp.bfloat16)

                combine(
                    [lambda j, cols, d=d: B3[d, q, j, :, cols]],
                    [(tile_view(RA, q, zat(sign), g), page_view(RL, zat(sign), g)) for g in range(8)],
                    write,
                )
                z_copy(q, d, 4).start()

        def hop3(q):
            for d in range(2):
                sign = 1 - 2 * d
                z_copy(q, d, 1).wait_recv()
                z_copy(q, d, 2).wait_recv()

                @pl.when(q >= RING)
                def _(d=d):
                    z_copy(q - RING, d, 3).wait_send()

                def write(j, cols, value, d=d):
                    C3[d, lax.rem(q, RING), j, :, cols] = value.astype(jnp.bfloat16)

                combine(
                    [],
                    [(tile_view(B2, d, q, i), page_view(L2, d, i)) for i in range(4)]
                    + [(tile_view(B2, d, q, 4 + i), page_view(L1, d, i)) for i in range(8)]
                    + [(tile_view(RA, q, zat(2 * sign), g), page_view(RL, zat(2 * sign), g)) for g in range(8)],
                    write,
                )
                z_copy(q, d, 3).start()

        def hop2(q):
            for d in range(2):
                z_copy(q, d, 0).wait_recv()
                z_copy(q, d, 1).start()
                z_copy(q, d, 2).start()

        def hop1(q):
            for i in range(1, 8):
                a_arrival(q, lax.rem(g_own + i, 8)).wait_recv()
            for d in range(2):
                z_copy(q, d, 0).start()

        def relay(q):
            for i in range(2):
                a_transit(q, i).wait_recv()
                a_forward(q, i).start()

        def form(q):
            for i in range(2):
                y_forward(q, i).wait_recv()
            left = jnp.concatenate(
                [own[:, q].reshape(3 * R, 2048), G[q].reshape(9 * R, 2048)], axis=0
            )
            for b in range(3):
                gram = dot_nt(left, own[b].reshape(PW, 2048))
                for p in range(12):
                    tiles[p * 3 + b] = (-gram[p * R : (p + 1) * R]).astype(jnp.bfloat16)
            for j in range(64):
                S[q, j // 8, j % 8] = tiles[seats_s[0, 0, j]]
            for i in range(2):
                a_transit(q, i).start()
            for i in range(5):
                a_direct(q, i).start()
            for zz in range(NZ):
                RA[q, zz, g_own] = S[q, g_own, zz]

        def labels_on():
            for i in range(1, 8):
                label_arrival(lax.rem(g_own + i, 8)).wait_recv()
            for d in range(2):
                for i in range(2):
                    label_z(d, i).start()

        def labels_in():
            for d in range(2):
                for i in range(2):
                    label_z(d, i).wait_recv()

        def lead(q):
            for i in range(2):
                y_direct(q, i).start()

        pl.when(step == 3)(labels_in)
        stage(5, finish)
        stage(4, hop4)
        stage(3, hop3)
        stage(2, hop2)
        stage(0, form)

        @pl.when(step + 1 < NQ)
        def _():
            gather_chunk(step + 1)

        @pl.when(step + 3 < NQ)
        def _():
            lead(step + 3)

        stage(1, hop1)
        stage(0, relay)
        pl.when(step == 0)(labels_on)
        return carry

    lax.fori_loop(0, NQ + 5, tick, 0)

    def drain(q, carry):
        for i in range(2):
            y_direct(q, i).wait_send()
            y_forward(q, i).wait_send()
            a_transit(q, i).wait_send()
            a_forward(q, i).wait_send()
        for i in range(5):
            a_direct(q, i).wait_send()
        for d in range(2):
            for h in range(3):
                z_copy(q, d, h).wait_send()
        return carry

    lax.fori_loop(0, NQ, drain, 0)
    for q in range(NQ - RING, NQ):
        for d in range(2):
            for h in (3, 4):
                z_copy(q, d, h).wait_send()
    for i in range(7):
        label_group(i).wait_send()
    for d in range(2):
        for i in range(2):
            label_z(d, i).wait_send()


def shards(coupling, panel_inv, a_ib, owner, slot, base):
    vmem = pl.BlockSpec(memory_space=pltpu.VMEM)
    smem = pl.BlockSpec(memory_space=pltpu.SMEM)
    hbm = pl.BlockSpec(memory_space=pl.ANY)
    bf16, i32 = jnp.bfloat16, jnp.int32
    dma = pltpu.SemaphoreType.DMA
    result = pl.pallas_call(
        schur_kernel,
        out_shape=jax.ShapeDtypeStruct((16, PW, PW), bf16),
        in_specs=[smem, smem, hbm, hbm, hbm, hbm],
        out_specs=vmem,
        scratch_shapes=[
            pltpu.VMEM((28, PW, PW), bf16),
            pltpu.VMEM((8, PW, PW), jnp.float32),
            pltpu.VMEM((2048, 768), bf16),
            pltpu.VMEM((16, PW, PW), bf16),
            pltpu.VMEM((3, NQ, R, 2048), bf16),
            pltpu.VMEM((2, 8, 128), i32),
            pltpu.SMEM((2, 8, 128), i32),
            pltpu.VMEM((8, 8, 8, 128), i32),
            pltpu.VMEM((NQ, 3, 3, R, 2048), bf16),
            pltpu.VMEM((NQ, 8, 8, R, PW), bf16),
            pltpu.VMEM((NQ, 8, 8, R, PW), bf16),
            pltpu.VMEM((NQ, 2, 8, R, PW), bf16),
            pltpu.VMEM((2, NQ, 4, R, PW), bf16),
            pltpu.VMEM((2, NQ, 12, R, PW), bf16),
            pltpu.VMEM((2, NQ, 16, R, PW), bf16),
            pltpu.VMEM((2, NQ, 16, R, PW), bf16),
            pltpu.VMEM((2, RING, 16, R, PW), bf16),
            pltpu.VMEM((2, RING, 16, R, PW), bf16),
            pltpu.VMEM((37, R, PW), bf16),
            pltpu.VMEM((8, 8, 8, 128), i32),
            pltpu.VMEM((2, 8, 8, 128), i32),
            pltpu.VMEM((2, 4, 8, 128), i32),
            dma((9, 3)),
            dma((NQ, 4)), dma((NQ, 4)),
            dma((NQ, 7)), dma((NQ, 2)), dma((NQ, 8)), dma((NQ, 2)),
            dma((NQ, 10)), dma((NQ, 10)),
            dma((11,)), dma((8,)), dma((4,)),
        ],
        compiler_params=pltpu.CompilerParams(
            collective_id=0, has_side_effects=True, vmem_limit_bytes=VMEM_LIMIT
        ),
        name="schur",
    )(
        owner.transpose(2, 0, 1),
        slot.transpose(2, 0, 1),
        coupling[0],
        panel_inv[0],
        a_ib[0],
        base[0],
    )
    return result[None]


def solution(mesh):
    placed = (
        P("sub", None, None, None),
        P("sub", None, None, None),
        P("sub", None, "tile"),
        P("sub", None, "tile"),
        P("sub", None, "tile"),
        P("sub", "tile", None, None),
    )
    return jax.shard_map(
        shards, mesh=mesh, in_specs=placed, out_specs=P("sub", "tile", None, None), check_vma=False
    )
```

```python
import functools

import jax
import jax.numpy as jnp
from jax import lax
from jax.experimental import pallas as pl
from jax.experimental.pallas import tpu as pltpu
from jax.sharding import PartitionSpec as P

MESH = pl.DeviceIdType.MESH
NX, NZ, NC, NY = 4, 8, 2, 4
PW = 256
NQ = 16
R = PW // NQ
FIRST = 4
RING = 4
VMEM_LIMIT = 67043328
NT = (((1,), (1,)), ((), ()))


def dot_nt(left, right):
    return lax.dot_general(left, right, NT, preferred_element_type=jnp.float32)


def split_hi_lo(value):
    high = value.astype(jnp.bfloat16)
    low = (value - high.astype(jnp.float32)).astype(jnp.bfloat16)
    return high, low


def combine(dense, tiles, write):
    for half in range(2):
        cols = slice(half * 128, half * 128 + 128)
        acc = [None] * 16
        for view in dense:
            for j in range(16):
                x = view(j, cols).astype(jnp.float32)
                acc[j] = x if acc[j] is None else acc[j] + x
        for view, page in tiles:
            x = view(cols).astype(jnp.float32)
            lab = page()
            lab = jnp.concatenate([lab] * (R // 8), axis=0)
            for j in range(16):
                term = jnp.where(lab == j, x, 0.0)
                acc[j] = term if acc[j] is None else acc[j] + term
        for j in range(16):
            write(j, cols, acc[j])


def schur_kernel(
    owner_s, slot_s, c_hbm, inv_hbm, a_hbm, base_hbm, out,
    c_v, inv_v, a_v, base, own, seats_v, seats_s, pages,
    G, S, RA, T, B1, B2, B3, B4, C3, C4, tiles, RL, L1, L2,
    ld, ss, ry, ra, rt, sz, rz, sl, rl, rlz,
):
    s = lax.axis_index("sub")
    t = lax.axis_index("tile")
    x, z, c = s // 16, lax.rem(s // 2, NZ), lax.rem(s, 2)
    g_own = x * 2 + c

    def at(dx, dz, core, dt):
        xx = lax.rem(x + dx + NX, NX)
        zz = lax.rem(z + dz + NZ, NZ)
        return ((xx * NZ + zz) * NC + core, lax.rem(t + dt + NY, NY))

    def group(dx, core):
        return lax.rem(x + dx + NX, NX) * 2 + core

    def ring(q):
        return lax.rem(q, RING)

    def zat(dz):
        return lax.rem(z + dz + NZ, NZ)

    def rc(src, dst, ss, rs, dev):
        return pltpu.make_async_remote_copy(
            src_ref=src, dst_ref=dst, send_sem=ss, recv_sem=rs, device_id=dev, device_id_type=MESH
        )

    direct = [(1, 0), (1, 1), (-1, 0), (-1, 1), (0, 1 - c)]
    two = [(2, 0), (2, 1)]

    def y_direct(q, i):
        return rc(own.at[:, q], G.at[q, i], ss.at[0], ry.at[ring(q), i], at(0, 0, c, (1, -1)[i]))

    def y_forward(q, i):
        lanes = pl.ds(i * 1024, 1024)
        return rc(
            G.at[q, i, :, :, lanes], G.at[q, 2, :, :, lanes],
            ss.at[0], ry.at[ring(q), 2 + i], at(0, 0, c, (1, -1)[i]),
        )

    def a_direct(q, i):
        dx, core = direct[i]
        return rc(
            S.at[q, group(dx, core)], RA.at[q, :, g_own], ss.at[1], ra.at[ring(q), g_own], at(dx, 0, core, 0)
        )

    def a_transit(q, i):
        return rc(
            S.at[q, group(2, i)], T.at[q, i], ss.at[1], rt.at[ring(q), i], at((1, -1)[i], 0, c, 0)
        )

    def a_forward(q, i):
        src_g = group((-1, 1)[i], c)
        return rc(
            T.at[q, i], RA.at[q, :, src_g], ss.at[1], ra.at[ring(q), src_g], at((1, -1)[i], 0, i, 0)
        )

    def a_arrival(q, g):
        return rc(S.at[q, g], RA.at[q, :, g], ss.at[1], ra.at[ring(q), g], at(0, 0, 1 - c, 0))

    def z_copy(q, d, h):
        sign = 1 - 2 * d
        dev = at(0, sign, c, 0)
        send = ss.at[2] if h < 3 else sz.at[ring(q), d * 2 + h - 3]
        if h == 0:
            src, dst = RA.at[q, zat(4), pl.ds(4 * d, 4)], B1.at[d, q]
        elif h == 1:
            src, dst = B1.at[d, q], B2.at[d, q, pl.ds(0, 4)]
        elif h == 2:
            src, dst = RA.at[q, zat(3 * sign)], B2.at[d, q, pl.ds(4, 8)]
        elif h == 3:
            src, dst = C3.at[d, ring(q)], B3.at[d, q]
        else:
            src, dst = C4.at[d, ring(q)], B4.at[d, q]
        return rc(src, dst, send, rz.at[ring(q), d * 5 + h], dev)

    def label_group(i):
        dx, core = (direct + two)[i]
        return rc(pages.at[group(dx, core)], RL.at[:, g_own], sl.at[i], rl.at[g_own], at(dx, 0, core, 0))

    def label_arrival(g):
        return rc(pages.at[g], RL.at[:, g], sl.at[0], rl.at[g], at(0, 0, 1 - c, 0))

    def label_z(d, i):
        sign = 1 - 2 * d
        if i == 0:
            src, dst = RL.at[zat(3 * sign)], L1.at[d]
        else:
            src, dst = RL.at[zat(4), pl.ds(4 * d, 4)], L2.at[d]
        return rc(src, dst, sl.at[7 + 2 * d + i], rlz.at[2 * d + i], at(0, sign * (1 + i), c, 0))

    def loads(k):
        rows = pl.ds(k * PW, PW)
        copies = [
            pltpu.make_async_copy(a_hbm.at[rows], a_v.at[rows], ld.at[k, 0]),
            pltpu.make_async_copy(inv_hbm.at[k], inv_v.at[k], ld.at[k, 1]),
        ]
        if k:
            blocks = pl.ds(k * (k - 1) // 2, k)
            copies.append(pltpu.make_async_copy(c_hbm.at[blocks], c_v.at[blocks], ld.at[k, 2]))
        return copies

    def solve_panel(k, first, last):
        count = 3 * (last - first) * R
        cols = slice(k * PW, (k + 1) * PW)
        target = own[:, first:last, :, cols].reshape(count, PW).astype(jnp.float32)
        if k:
            start = k * (k - 1) // 2
            joined = jnp.concatenate([c_v[start + m] for m in range(k)], axis=1)
            target = target - dot_nt(own[:, first:last, :, : k * PW].reshape(count, k * PW), joined)
        t_hi, t_lo = split_hi_lo(target)
        i_hi, i_lo = split_hi_lo(inv_v[k])
        solved = dot_nt(
            jnp.concatenate([t_hi, t_hi, t_lo], axis=1), jnp.concatenate([i_hi, i_lo, i_hi], axis=1)
        )
        own[:, first:last, :, cols] = solved.astype(jnp.bfloat16).reshape(3, last - first, R, PW)

    def gather_chunk(q):
        for i in range(2):
            y_direct(q, i).wait_recv()
            y_forward(q, i).start()

    for k in range(8):
        for copy in loads(k):
            copy.start()
    base_load = pltpu.make_async_copy(base_hbm, base, ld.at[8, 0])
    base_load.start()

    barrier = pltpu.get_barrier_semaphore()
    peers = [at(dx, 0, core, 0) for dx, core in direct + two]
    peers += [at(0, dz, c, 0) for dz in (1, -1, 2, -2)] + [at(0, 0, c, dt) for dt in (1, -1)]
    for dev in peers:
        pl.semaphore_signal(barrier, inc=1, device_id=dev, device_id_type=MESH)

    for k in range(8):
        for copy in loads(k):
            copy.wait()
        cols = slice(k * PW, (k + 1) * PW)
        rows = a_v[cols, :].T
        own[:, :, :, cols] = rows.reshape(3, NQ, R, PW)
        solve_panel(k, 0, FIRST)
    pl.semaphore_wait(barrier, len(peers))
    for i in range(2):
        y_direct(0, i).start()

    lane = lax.broadcasted_iota(jnp.int32, (8, 128), 1)
    seat_tile = jnp.full((8, 128), 36, jnp.int32)
    seat_slot = jnp.full((8, 128), -1, jnp.int32)
    for a in range(12):
        d = lax.rem(a // 3 - t + NY, NY)
        rel = jnp.where(d == 0, 0, jnp.where(d == 3, 1, jnp.where(d == 1, 2, 3)))
        for b in range(3):
            o = owner_s[b, 0, a]
            seat = ((o // 16) * 2 + lax.rem(o, 2)) * 8 + lax.rem(o // 2, 8)
            here = lane == seat
            seat_tile = jnp.where(here, (rel * 3 + a % 3) * 3 + b, seat_tile)
            seat_slot = jnp.where(here, slot_s[b, 0, a], seat_slot)
    seats_v[0] = seat_tile
    seats_v[1] = seat_slot
    to_scalar = pltpu.make_async_copy(seats_v, seats_s, ld.at[8, 1])
    to_scalar.start()
    to_scalar.wait()
    for j in range(64):
        pages[j // 8, j % 8] = jnp.full((8, 128), seats_s[1, 0, j], jnp.int32)
    for i in range(7):
        label_group(i).start()
    for k in range(8):
        solve_panel(k, FIRST, NQ)
        if k == 5:
            gather_chunk(0)
            for q in (1, 2):
                for i in range(2):
                    y_direct(q, i).start()
    tiles[36] = jnp.zeros((R, PW), jnp.bfloat16)
    for zz in range(NZ):
        RL[zz, g_own] = pages[g_own, zz]
    base_load.wait()

    def tile_view(ref, *index):
        return lambda cols: ref[(*index, slice(None), cols)]

    def page_view(ref, *index):
        return lambda: ref[index]

    def tick(step, carry):
        def stage(lag, run):
            q = step - lag

            @pl.when(jnp.logical_and(q >= 0, q < NQ))
            def _():
                run(q)

        def finish(q):
            for d in range(2):
                z_copy(q, d, 4).wait_recv()
            rows = pl.ds(pl.multiple_of(q * R, R), R)

            def write(j, cols, value):
                out[j, rows, cols] = value.astype(jnp.bfloat16)

            combine(
                [lambda j, cols: base[j, rows, cols]]
                + [lambda j, cols, d=d: B4[d, q, j, :, cols] for d in range(2)],
                [(tile_view(RA, q, z, g), page_view(RL, z, g)) for g in range(8)],
                write,
            )

        def hop4(q):
            for d in range(2):
                sign = 1 - 2 * d
                z_copy(q, d, 3).wait_recv()

                @pl.when(q >= RING)
                def _(d=d):
                    z_copy(q - RING, d, 4).wait_send()

                def write(j, cols, value, d=d):
                    C4[d, ring(q), j, :, cols] = value.astype(jnp.bfloat16)

                combine(
                    [lambda j, cols, d=d: B3[d, q, j, :, cols]],
                    [(tile_view(RA, q, zat(sign), g), page_view(RL, zat(sign), g)) for g in range(8)],
                    write,
                )
                z_copy(q, d, 4).start()

        def hop3(q):
            for d in range(2):
                sign = 1 - 2 * d
                z_copy(q, d, 1).wait_recv()
                z_copy(q, d, 2).wait_recv()

                @pl.when(q >= RING)
                def _(d=d):
                    z_copy(q - RING, d, 3).wait_send()

                def write(j, cols, value, d=d):
                    C3[d, ring(q), j, :, cols] = value.astype(jnp.bfloat16)

                combine(
                    [],
                    [(tile_view(B2, d, q, i), page_view(L2, d, i)) for i in range(4)]
                    + [(tile_view(B2, d, q, 4 + i), page_view(L1, d, i)) for i in range(8)]
                    + [(tile_view(RA, q, zat(2 * sign), g), page_view(RL, zat(2 * sign), g)) for g in range(8)],
                    write,
                )
                z_copy(q, d, 3).start()

        def hop2(q):
            for d in range(2):
                z_copy(q, d, 0).wait_recv()
                z_copy(q, d, 1).start()
                z_copy(q, d, 2).start()

        def hop1(q):
            for i in range(1, 8):
                a_arrival(q, lax.rem(g_own + i, 8)).wait_recv()
            for d in range(2):
                z_copy(q, d, 0).start()

        def relay(q):
            for i in range(2):
                a_transit(q, i).wait_recv()
                a_forward(q, i).start()

        def form(q):
            for i in range(2):
                y_forward(q, i).wait_recv()
            left = jnp.concatenate(
                [own[:, q].reshape(3 * R, 2048), G[q].reshape(9 * R, 2048)], axis=0
            )
            for b in range(3):
                gram = dot_nt(left, own[b].reshape(PW, 2048))
                for p in range(12):
                    tiles[p * 3 + b] = (-gram[p * R : (p + 1) * R]).astype(jnp.bfloat16)
            for j in range(64):
                S[q, j // 8, j % 8] = tiles[seats_s[0, 0, j]]
            for i in range(2):
                a_transit(q, i).start()
            for i in range(5):
                a_direct(q, i).start()
            for zz in range(NZ):
                RA[q, zz, g_own] = S[q, g_own, zz]

        def labels_on():
            for i in range(1, 8):
                label_arrival(lax.rem(g_own + i, 8)).wait_recv()
            for d in range(2):
                for i in range(2):
                    label_z(d, i).start()

        def labels_in():
            for d in range(2):
                for i in range(2):
                    label_z(d, i).wait_recv()

        def lead(q):
            for i in range(2):
                y_direct(q, i).start()

        pl.when(step == 3)(labels_in)
        stage(5, finish)
        stage(4, hop4)
        stage(3, hop3)
        stage(2, hop2)
        stage(0, form)

        @pl.when(step + 1 < NQ)
        def _():
            gather_chunk(step + 1)

        @pl.when(step + 3 < NQ)
        def _():
            lead(step + 3)

        stage(1, hop1)
        stage(0, relay)
        pl.when(step == 0)(labels_on)
        return carry

    lax.fori_loop(0, NQ + 5, tick, 0)

    for i, whole in enumerate((G, G, B3)):
        rc(whole, whole, ss.at[i], ss.at[i], at(0, 0, 1 - c, 0)).wait_send()
    for q in range(NQ - RING, NQ):
        for d in range(2):
            for h in (3, 4):
                z_copy(q, d, h).wait_send()
    for i in range(7):
        label_group(i).wait_send()
    for d in range(2):
        for i in range(2):
            label_z(d, i).wait_send()


def shards(coupling, panel_inv, a_ib, owner, slot, base):
    vmem = pl.BlockSpec(memory_space=pltpu.VMEM)
    smem = pl.BlockSpec(memory_space=pltpu.SMEM)
    hbm = pl.BlockSpec(memory_space=pl.ANY)
    bf16, i32 = jnp.bfloat16, jnp.int32
    dma = pltpu.SemaphoreType.DMA
    result = pl.pallas_call(
        schur_kernel,
        out_shape=jax.ShapeDtypeStruct((16, PW, PW), bf16),
        in_specs=[smem, smem, hbm, hbm, hbm, hbm],
        out_specs=vmem,
        scratch_shapes=[
            pltpu.VMEM((28, PW, PW), bf16),
            pltpu.VMEM((8, PW, PW), jnp.float32),
            pltpu.VMEM((2048, 768), bf16),
            pltpu.VMEM((16, PW, PW), bf16),
            pltpu.VMEM((3, NQ, R, 2048), bf16),
            pltpu.VMEM((2, 8, 128), i32),
            pltpu.SMEM((2, 8, 128), i32),
            pltpu.VMEM((8, 8, 8, 128), i32),
            pltpu.VMEM((NQ, 3, 3, R, 2048), bf16),
            pltpu.VMEM((NQ, 8, 8, R, PW), bf16),
            pltpu.VMEM((NQ, 8, 8, R, PW), bf16),
            pltpu.VMEM((NQ, 2, 8, R, PW), bf16),
            pltpu.VMEM((2, NQ, 4, R, PW), bf16),
            pltpu.VMEM((2, NQ, 12, R, PW), bf16),
            pltpu.VMEM((2, NQ, 16, R, PW), bf16),
            pltpu.VMEM((2, NQ, 16, R, PW), bf16),
            pltpu.VMEM((2, RING, 16, R, PW), bf16),
            pltpu.VMEM((2, RING, 16, R, PW), bf16),
            pltpu.VMEM((37, R, PW), bf16),
            pltpu.VMEM((8, 8, 8, 128), i32),
            pltpu.VMEM((2, 8, 8, 128), i32),
            pltpu.VMEM((2, 4, 8, 128), i32),
            dma((9, 3)),
            dma((3,)),
            dma((RING, 4)), dma((RING, 8)), dma((RING, 2)),
            dma((RING, 4)), dma((RING, 10)),
            dma((11,)), dma((8,)), dma((4,)),
        ],
        compiler_params=pltpu.CompilerParams(
            collective_id=0, has_side_effects=True, vmem_limit_bytes=VMEM_LIMIT
        ),
        name="schur",
    )(
        owner.transpose(2, 0, 1),
        slot.transpose(2, 0, 1),
        coupling[0],
        panel_inv[0],
        a_ib[0],
        base[0],
    )
    return result[None]


def solution(mesh):
    placed = (
        P("sub", None, None, None),
        P("sub", None, None, None),
        P("sub", None, "tile"),
        P("sub", None, "tile"),
        P("sub", None, "tile"),
        P("sub", "tile", None, None),
    )
    return jax.shard_map(
        shards, mesh=mesh, in_specs=placed, out_specs=P("sub", "tile", None, None), check_vma=False
    )
```

```python
import functools

import jax
import jax.numpy as jnp
from jax import lax
from jax.experimental import pallas as pl
from jax.experimental.pallas import tpu as pltpu
from jax.sharding import PartitionSpec as P

MESH = pl.DeviceIdType.MESH
NX, NZ, NC, NY = 4, 8, 2, 4
PW = 256
NQ = 16
R = PW // NQ
FIRST = 4
RING = 4
VMEM_LIMIT = 59 * 2**20
NT = (((1,), (1,)), ((), ()))


def dot_nt(left, right):
    return lax.dot_general(left, right, NT, preferred_element_type=jnp.float32)


def split_hi_lo(value):
    high = value.astype(jnp.bfloat16)
    low = (value - high.astype(jnp.float32)).astype(jnp.bfloat16)
    return high, low


def combine(dense, tiles, write):
    for half in range(2):
        cols = slice(half * 128, half * 128 + 128)
        acc = [None] * 16
        for view in dense:
            for j in range(16):
                x = view(j, cols).astype(jnp.float32)
                acc[j] = x if acc[j] is None else acc[j] + x
        for view, page in tiles:
            x = view(cols).astype(jnp.float32)
            lab = page()
            lab = jnp.concatenate([lab] * (R // 8), axis=0)
            for j in range(16):
                term = jnp.where(lab == j, x, 0.0)
                acc[j] = term if acc[j] is None else acc[j] + term
        for j in range(16):
            write(j, cols, acc[j])


def schur_kernel(
    owner_s, slot_s, c_hbm, inv_hbm, a_hbm, base_hbm, out,
    c_v, inv_v, a_v, base, own, seats_v, seats_s, pages,
    G, S, RA, T, B1, B2, B3, B4, C3, C4, tiles, RL, L1, L2,
    ld, ss, ry, ra, rt, sz, rz, sl, rl, rlz,
):
    s = lax.axis_index("sub")
    t = lax.axis_index("tile")
    x, z, c = s // 16, lax.rem(s // 2, NZ), lax.rem(s, 2)
    g_own = x * 2 + c

    def at(dx, dz, core, dt):
        xx = lax.rem(x + dx + NX, NX)
        zz = lax.rem(z + dz + NZ, NZ)
        return ((xx * NZ + zz) * NC + core, lax.rem(t + dt + NY, NY))

    def group(dx, core):
        return lax.rem(x + dx + NX, NX) * 2 + core

    def ring(q):
        return lax.rem(q, RING)

    def zat(dz):
        return lax.rem(z + dz + NZ, NZ)

    def rc(src, dst, ss, rs, dev):
        return pltpu.make_async_remote_copy(
            src_ref=src, dst_ref=dst, send_sem=ss, recv_sem=rs, device_id=dev, device_id_type=MESH
        )

    direct = [(1, 0), (1, 1), (-1, 0), (-1, 1), (0, 1 - c)]
    two = [(2, 0), (2, 1)]

    def y_direct(q, i, part):
        lanes = pl.ds(1024 * (i if part == 0 else 1 - i), 1024)
        return rc(
            own.at[:, q, :, lanes], G.at[q, i, :, :, lanes],
            ss.at[0], ry.at[ring(q), 2 * i + part], at(0, 0, c, (1, -1)[i]),
        )

    def y_forward(q, i):
        lanes = pl.ds(i * 1024, 1024)
        return rc(
            G.at[q, i, :, :, lanes], G.at[q, 2, :, :, lanes],
            ss.at[0], ry.at[ring(q), 4 + i], at(0, 0, c, (1, -1)[i]),
        )

    def a_direct(q, i):
        dx, core = direct[i]
        return rc(
            S.at[q, group(dx, core)], RA.at[q, :, g_own], ss.at[1], ra.at[ring(q), g_own], at(dx, 0, core, 0)
        )

    def a_transit(q, i):
        return rc(
            S.at[q, group(2, i)], T.at[q, i], ss.at[1], rt.at[ring(q), i], at((1, -1)[i], 0, c, 0)
        )

    def a_forward(q, i):
        src_g = group((-1, 1)[i], c)
        return rc(
            T.at[q, i], RA.at[q, :, src_g], ss.at[1], ra.at[ring(q), src_g], at((1, -1)[i], 0, i, 0)
        )

    def a_arrival(q, g):
        return rc(S.at[q, g], RA.at[q, :, g], ss.at[1], ra.at[ring(q), g], at(0, 0, 1 - c, 0))

    def z_copy(q, d, h):
        sign = 1 - 2 * d
        dev = at(0, sign, c, 0)
        send = ss.at[2] if h < 3 else sz.at[ring(q), d * 2 + h - 3]
        if h == 0:
            src, dst = RA.at[q, zat(4), pl.ds(4 * d, 4)], B1.at[d, q]
        elif h == 1:
            src, dst = B1.at[d, q], B2.at[d, q, pl.ds(0, 4)]
        elif h == 2:
            src, dst = RA.at[q, zat(3 * sign)], B2.at[d, q, pl.ds(4, 8)]
        elif h == 3:
            src, dst = C3.at[d, ring(q)], B3.at[d, q]
        else:
            src, dst = C4.at[d, ring(q)], B4.at[d, q]
        return rc(src, dst, send, rz.at[ring(q), d * 5 + h], dev)

    def label_group(i):
        dx, core = (direct + two)[i]
        return rc(pages.at[group(dx, core)], RL.at[:, g_own], sl.at[i], rl.at[g_own], at(dx, 0, core, 0))

    def label_arrival(g):
        return rc(pages.at[g], RL.at[:, g], sl.at[0], rl.at[g], at(0, 0, 1 - c, 0))

    def label_z(d, i):
        sign = 1 - 2 * d
        if i == 0:
            src, dst = RL.at[zat(3 * sign)], L1.at[d]
        else:
            src, dst = RL.at[zat(4), pl.ds(4 * d, 4)], L2.at[d]
        return rc(src, dst, sl.at[7 + 2 * d + i], rlz.at[2 * d + i], at(0, sign * (1 + i), c, 0))

    def loads(k):
        rows = pl.ds(k * PW, PW)
        copies = [
            pltpu.make_async_copy(a_hbm.at[rows], a_v.at[rows], ld.at[k, 0]),
            pltpu.make_async_copy(inv_hbm.at[k], inv_v.at[k], ld.at[k, 1]),
        ]
        if k:
            blocks = pl.ds(k * (k - 1) // 2, k)
            copies.append(pltpu.make_async_copy(c_hbm.at[blocks], c_v.at[blocks], ld.at[k, 2]))
        return copies

    def solve_panel(k, first, last):
        count = 3 * (last - first) * R
        cols = slice(k * PW, (k + 1) * PW)
        target = own[:, first:last, :, cols].reshape(count, PW).astype(jnp.float32)
        if k:
            start = k * (k - 1) // 2
            joined = jnp.concatenate([c_v[start + m] for m in range(k)], axis=1)
            target = target - dot_nt(own[:, first:last, :, : k * PW].reshape(count, k * PW), joined)
        t_hi, t_lo = split_hi_lo(target)
        i_hi, i_lo = split_hi_lo(inv_v[k])
        solved = dot_nt(
            jnp.concatenate([t_hi, t_hi, t_lo], axis=1), jnp.concatenate([i_hi, i_lo, i_hi], axis=1)
        )
        own[:, first:last, :, cols] = solved.astype(jnp.bfloat16).reshape(3, last - first, R, PW)

    def lead(q):
        for part in range(2):
            for i in range(2):
                y_direct(q, i, part).start()

    def gather_chunk(q):
        for i in range(2):
            y_direct(q, i, 0).wait_recv()
            y_forward(q, i).start()

    for k in range(8):
        for copy in loads(k):
            copy.start()
    base_load = pltpu.make_async_copy(base_hbm, base, ld.at[8, 0])

    barrier = pltpu.get_barrier_semaphore()
    peers = [at(dx, 0, core, 0) for dx, core in direct + two]
    peers += [at(0, dz, c, 0) for dz in (1, -1, 2, -2)] + [at(0, 0, c, dt) for dt in (1, -1)]
    for dev in peers:
        pl.semaphore_signal(barrier, inc=1, device_id=dev, device_id_type=MESH)

    for k in range(8):
        for copy in loads(k):
            copy.wait()
        cols = slice(k * PW, (k + 1) * PW)
        rows = a_v[cols, :].T
        own[:, :, :, cols] = rows.reshape(3, NQ, R, PW)
        solve_panel(k, 0, FIRST)
    base_load.start()
    pl.semaphore_wait(barrier, len(peers))
    lead(0)

    lane = lax.broadcasted_iota(jnp.int32, (8, 128), 1)
    seat_tile = jnp.full((8, 128), 36, jnp.int32)
    seat_slot = jnp.full((8, 128), -1, jnp.int32)
    for a in range(12):
        d = lax.rem(a // 3 - t + NY, NY)
        rel = jnp.where(d == 0, 0, jnp.where(d == 3, 1, jnp.where(d == 1, 2, 3)))
        for b in range(3):
            o = owner_s[b, 0, a]
            seat = ((o // 16) * 2 + lax.rem(o, 2)) * 8 + lax.rem(o // 2, 8)
            here = lane == seat
            seat_tile = jnp.where(here, (rel * 3 + a % 3) * 3 + b, seat_tile)
            seat_slot = jnp.where(here, slot_s[b, 0, a], seat_slot)
    seats_v[0] = seat_tile
    seats_v[1] = seat_slot
    to_scalar = pltpu.make_async_copy(seats_v, seats_s, ld.at[8, 1])
    to_scalar.start()
    to_scalar.wait()
    for j in range(64):
        pages[j // 8, j % 8] = jnp.full((8, 128), seats_s[1, 0, j], jnp.int32)
    for i in range(7):
        label_group(i).start()
    for k in range(8):
        solve_panel(k, FIRST, NQ)
        if k == 5:
            gather_chunk(0)
            lead(1)
    tiles[36] = jnp.zeros((R, PW), jnp.bfloat16)
    for zz in range(NZ):
        RL[zz, g_own] = pages[g_own, zz]
    base_load.wait()

    def tile_view(ref, *index):
        return lambda cols: ref[(*index, slice(None), cols)]

    def page_view(ref, *index):
        return lambda: ref[index]

    def tick(step, carry):
        def stage(lag, run):
            q = step - lag

            @pl.when(jnp.logical_and(q >= 0, q < NQ))
            def _():
                run(q)

        def finish(q):
            for d in range(2):
                z_copy(q, d, 4).wait_recv()
            rows = pl.ds(pl.multiple_of(q * R, R), R)

            def write(j, cols, value):
                out[j, rows, cols] = value.astype(jnp.bfloat16)

            combine(
                [lambda j, cols: base[j, rows, cols]]
                + [lambda j, cols, d=d: B4[d, q, j, :, cols] for d in range(2)],
                [(tile_view(RA, q, z, g), page_view(RL, z, g)) for g in range(8)],
                write,
            )

        def hop4(q):
            for d in range(2):
                sign = 1 - 2 * d
                z_copy(q, d, 3).wait_recv()

                @pl.when(q >= RING)
                def _(d=d):
                    z_copy(q - RING, d, 4).wait_send()

                def write(j, cols, value, d=d):
                    C4[d, ring(q), j, :, cols] = value.astype(jnp.bfloat16)

                combine(
                    [lambda j, cols, d=d: B3[d, q, j, :, cols]],
                    [(tile_view(RA, q, zat(sign), g), page_view(RL, zat(sign), g)) for g in range(8)],
                    write,
                )
                z_copy(q, d, 4).start()

        def hop3(q):
            for d in range(2):
                sign = 1 - 2 * d
                z_copy(q, d, 1).wait_recv()
                z_copy(q, d, 2).wait_recv()

                @pl.when(q >= RING)
                def _(d=d):
                    z_copy(q - RING, d, 3).wait_send()

                def write(j, cols, value, d=d):
                    C3[d, ring(q), j, :, cols] = value.astype(jnp.bfloat16)

                combine(
                    [],
                    [(tile_view(B2, d, q, i), page_view(L2, d, i)) for i in range(4)]
                    + [(tile_view(B2, d, q, 4 + i), page_view(L1, d, i)) for i in range(8)]
                    + [(tile_view(RA, q, zat(2 * sign), g), page_view(RL, zat(2 * sign), g)) for g in range(8)],
                    write,
                )
                z_copy(q, d, 3).start()

        def hop2(q):
            for d in range(2):
                z_copy(q, d, 0).wait_recv()
                z_copy(q, d, 1).start()
                z_copy(q, d, 2).start()

        def hop1(q):
            for i in range(1, 8):
                a_arrival(q, lax.rem(g_own + i, 8)).wait_recv()
            for d in range(2):
                z_copy(q, d, 0).start()

        def relay(q):
            for i in range(2):
                a_transit(q, i).wait_recv()
                a_forward(q, i).start()

        def form(q):
            for i in range(2):
                y_direct(q, i, 1).wait_recv()
                y_forward(q, i).wait_recv()
            left = jnp.concatenate(
                [own[:, q].reshape(3 * R, 2048), G[q].reshape(9 * R, 2048)], axis=0
            )
            for b in range(3):
                gram = dot_nt(left, own[b].reshape(PW, 2048))
                for p in range(12):
                    tiles[p * 3 + b] = (-gram[p * R : (p + 1) * R]).astype(jnp.bfloat16)
            for j in range(64):
                S[q, j // 8, j % 8] = tiles[seats_s[0, 0, j]]
            for i in range(2):
                a_transit(q, i).start()
            for i in range(5):
                a_direct(q, i).start()
            for zz in range(NZ):
                RA[q, zz, g_own] = S[q, g_own, zz]

        def labels_on():
            for i in range(1, 8):
                label_arrival(lax.rem(g_own + i, 8)).wait_recv()
            for d in range(2):
                for i in range(2):
                    label_z(d, i).start()

        def labels_in():
            for d in range(2):
                for i in range(2):
                    label_z(d, i).wait_recv()

        pl.when(step == 2)(labels_in)
        stage(2, hop2)
        pl.when(step == 1)(labels_on)
        stage(1, relay)
        stage(6, finish)

        @pl.when(step + 1 < NQ)
        def _():
            gather_chunk(step + 1)

        @pl.when(step + 2 < NQ)
        def _():
            lead(step + 2)

        stage(0, form)
        stage(4, hop4)
        stage(1, hop1)
        stage(2, hop3)
        return carry

    lax.fori_loop(0, NQ + 6, tick, 0)

    for i, whole in enumerate((G, G, B3)):
        rc(whole, whole, ss.at[i], ss.at[i], at(0, 0, 1 - c, 0)).wait_send()
    for q in range(NQ - RING, NQ):
        for d in range(2):
            for h in (3, 4):
                z_copy(q, d, h).wait_send()
    for i in range(7):
        label_group(i).wait_send()
    for d in range(2):
        for i in range(2):
            label_z(d, i).wait_send()


def shards(coupling, panel_inv, a_ib, owner, slot, base):
    vmem = pl.BlockSpec(memory_space=pltpu.VMEM)
    smem = pl.BlockSpec(memory_space=pltpu.SMEM)
    hbm = pl.BlockSpec(memory_space=pl.ANY)
    bf16, i32 = jnp.bfloat16, jnp.int32
    dma = pltpu.SemaphoreType.DMA
    result = pl.pallas_call(
        schur_kernel,
        out_shape=pltpu.VMEM((16, PW, PW), bf16),
        in_specs=[smem, smem, hbm, hbm, hbm, hbm],
        out_specs=vmem,
        scratch_shapes=[
            pltpu.VMEM((28, PW, PW), bf16),
            pltpu.VMEM((8, PW, PW), jnp.float32),
            pltpu.VMEM((2048, 768), bf16),
            pltpu.VMEM((16, PW, PW), bf16),
            pltpu.VMEM((3, NQ, R, 2048), bf16),
            pltpu.VMEM((2, 8, 128), i32),
            pltpu.SMEM((2, 8, 128), i32),
            pltpu.VMEM((8, 8, 8, 128), i32),
            pltpu.VMEM((NQ, 3, 3, R, 2048), bf16),
            pltpu.VMEM((NQ, 8, 8, R, PW), bf16),
            pltpu.VMEM((NQ, 8, 8, R, PW), bf16),
            pltpu.VMEM((NQ, 2, 8, R, PW), bf16),
            pltpu.VMEM((2, NQ, 4, R, PW), bf16),
            pltpu.VMEM((2, NQ, 12, R, PW), bf16),
            pltpu.VMEM((2, NQ, 16, R, PW), bf16),
            pltpu.VMEM((2, NQ, 16, R, PW), bf16),
            pltpu.VMEM((2, RING, 16, R, PW), bf16),
            pltpu.VMEM((2, RING, 16, R, PW), bf16),
            pltpu.VMEM((37, R, PW), bf16),
            pltpu.VMEM((8, 8, 8, 128), i32),
            pltpu.VMEM((2, 8, 8, 128), i32),
            pltpu.VMEM((2, 4, 8, 128), i32),
            dma((9, 3)),
            dma((3,)),
            dma((RING, 6)), dma((RING, 8)), dma((RING, 2)),
            dma((RING, 4)), dma((RING, 10)),
            dma((11,)), dma((8,)), dma((4,)),
        ],
        compiler_params=pltpu.CompilerParams(
            collective_id=0, has_side_effects=True, vmem_limit_bytes=VMEM_LIMIT
        ),
        name="schur",
    )(
        owner.transpose(2, 0, 1),
        slot.transpose(2, 0, 1),
        coupling[0],
        panel_inv[0],
        a_ib[0],
        base[0],
    )
    return result[None]


def solution(mesh):
    placed = (
        P("sub", None, None, None),
        P("sub", None, None, None),
        P("sub", None, "tile"),
        P("sub", None, "tile"),
        P("sub", None, "tile"),
        P("sub", "tile", None, None),
    )
    return jax.shard_map(
        shards, mesh=mesh, in_specs=placed, out_specs=P("sub", "tile", None, None), check_vma=False
    )
```

```python
import functools

import jax
import jax.numpy as jnp
from jax import lax
from jax.experimental import pallas as pl
from jax.experimental.pallas import tpu as pltpu
from jax.sharding import PartitionSpec as P

MESH = pl.DeviceIdType.MESH
NX, NZ, NC, NY = 4, 8, 2, 4
PW = 256
NQ = 16
R = PW // NQ
FIRST = 4
RING = 4
VMEM_LIMIT = 59 * 2**20
NT = (((1,), (1,)), ((), ()))


def dot_nt(left, right):
    return lax.dot_general(left, right, NT, preferred_element_type=jnp.float32)


def split_hi_lo(value):
    high = value.astype(jnp.bfloat16)
    low = (value - high.astype(jnp.float32)).astype(jnp.bfloat16)
    return high, low


def combine(dense, tiles, write):
    for half in range(2):
        cols = slice(half * 128, half * 128 + 128)
        acc = [None] * 16
        for view in dense:
            for j in range(16):
                x = view(j, cols).astype(jnp.float32)
                acc[j] = x if acc[j] is None else acc[j] + x
        for view, page in tiles:
            x = view(cols).astype(jnp.float32)
            lab = page()
            lab = jnp.concatenate([lab] * (R // 8), axis=0)
            for j in range(16):
                term = jnp.where(lab == j, x, 0.0)
                acc[j] = term if acc[j] is None else acc[j] + term
        for j in range(16):
            write(j, cols, acc[j])


def schur_kernel(
    owner_s, slot_s, c_hbm, inv_hbm, a_hbm, base_hbm, out,
    c_v, inv_v, a_v, base, own, seats_v, seats_s, pages,
    G, S, RA, T, B1, B2, B3, B4, C3, C4, tiles, RL, L1, L2,
    ld, ss, ry, ra, rt, sz, rz, sl, rl, rlz,
):
    s = lax.axis_index("sub")
    t = lax.axis_index("tile")
    x, z, c = s // 16, lax.rem(s // 2, NZ), lax.rem(s, 2)
    g_own = x * 2 + c

    def at(dx, dz, core, dt):
        xx = lax.rem(x + dx + NX, NX)
        zz = lax.rem(z + dz + NZ, NZ)
        return ((xx * NZ + zz) * NC + core, lax.rem(t + dt + NY, NY))

    def group(dx, core):
        return lax.rem(x + dx + NX, NX) * 2 + core

    def ring(q):
        return lax.rem(q, RING)

    def zat(dz):
        return lax.rem(z + dz + NZ, NZ)

    def rc(src, dst, ss, rs, dev):
        return pltpu.make_async_remote_copy(
            src_ref=src, dst_ref=dst, send_sem=ss, recv_sem=rs, device_id=dev, device_id_type=MESH
        )

    direct = [(1, 0), (1, 1), (-1, 0), (-1, 1), (0, 1 - c)]
    two = [(2, 0), (2, 1)]

    def y_direct(q, i, part):
        lanes = pl.ds(1024 * (i if part == 0 else 1 - i), 1024)
        return rc(
            own.at[:, q, :, lanes], G.at[q, i, :, :, lanes],
            ss.at[0], ry.at[ring(q), 2 * i + part], at(0, 0, c, (1, -1)[i]),
        )

    def y_forward(q, i):
        lanes = pl.ds(i * 1024, 1024)
        return rc(
            G.at[q, i, :, :, lanes], G.at[q, 2, :, :, lanes],
            ss.at[0], ry.at[ring(q), 4 + i], at(0, 0, c, (1, -1)[i]),
        )

    def a_direct(q, i):
        dx, core = direct[i]
        return rc(
            S.at[q, group(dx, core)], RA.at[q, :, g_own], ss.at[1], ra.at[ring(q), g_own], at(dx, 0, core, 0)
        )

    def a_transit(q, i):
        return rc(
            S.at[q, group(2, i)], T.at[q, i], ss.at[1], rt.at[ring(q), i], at((1, -1)[i], 0, c, 0)
        )

    def a_forward(q, i):
        src_g = group((-1, 1)[i], c)
        return rc(
            T.at[q, i], RA.at[q, :, src_g], ss.at[1], ra.at[ring(q), src_g], at((1, -1)[i], 0, i, 0)
        )

    def a_arrival(q, g):
        return rc(S.at[q, g], RA.at[q, :, g], ss.at[1], ra.at[ring(q), g], at(0, 0, 1 - c, 0))

    def z_copy(q, d, h):
        sign = 1 - 2 * d
        dev = at(0, sign, c, 0)
        send = ss.at[2] if h < 3 else sz.at[ring(q), d * 2 + h - 3]
        if h == 0:
            src, dst = RA.at[q, zat(4), pl.ds(4 * d, 4)], B1.at[d, q]
        elif h == 1:
            src, dst = B1.at[d, q], B2.at[d, q, pl.ds(0, 4)]
        elif h == 2:
            src, dst = RA.at[q, zat(3 * sign)], B2.at[d, q, pl.ds(4, 8)]
        elif h == 3:
            src, dst = C3.at[d, ring(q)], B3.at[d, q]
        else:
            src, dst = C4.at[d, ring(q)], B4.at[d, q]
        return rc(src, dst, send, rz.at[ring(q), d * 5 + h], dev)

    def label_group(i):
        dx, core = (direct + two)[i]
        return rc(pages.at[group(dx, core)], RL.at[:, g_own], sl.at[i], rl.at[g_own], at(dx, 0, core, 0))

    def label_arrival(g):
        return rc(pages.at[g], RL.at[:, g], sl.at[0], rl.at[g], at(0, 0, 1 - c, 0))

    def label_z(d, i):
        sign = 1 - 2 * d
        if i == 0:
            src, dst = RL.at[zat(3 * sign)], L1.at[d]
        else:
            src, dst = RL.at[zat(4), pl.ds(4 * d, 4)], L2.at[d]
        return rc(src, dst, sl.at[7 + 2 * d + i], rlz.at[2 * d + i], at(0, sign * (1 + i), c, 0))

    def loads(k):
        rows = pl.ds(k * PW, PW)
        copies = [
            pltpu.make_async_copy(a_hbm.at[rows], a_v.at[rows], ld.at[k, 0]),
            pltpu.make_async_copy(inv_hbm.at[k], inv_v.at[k], ld.at[k, 1]),
        ]
        if k:
            blocks = pl.ds(k * (k - 1) // 2, k)
            copies.append(pltpu.make_async_copy(c_hbm.at[blocks], c_v.at[blocks], ld.at[k, 2]))
        return copies

    def solve_panel(k, first, last):
        count = 3 * (last - first) * R
        cols = slice(k * PW, (k + 1) * PW)
        target = own[:, first:last, :, cols].reshape(count, PW).astype(jnp.float32)
        if k:
            start = k * (k - 1) // 2
            joined = jnp.concatenate([c_v[start + m] for m in range(k)], axis=1)
            target = target - dot_nt(own[:, first:last, :, : k * PW].reshape(count, k * PW), joined)
        t_hi, t_lo = split_hi_lo(target)
        i_hi, i_lo = split_hi_lo(inv_v[k])
        solved = dot_nt(
            jnp.concatenate([t_hi, t_hi, t_lo], axis=1), jnp.concatenate([i_hi, i_lo, i_hi], axis=1)
        )
        own[:, first:last, :, cols] = solved.astype(jnp.bfloat16).reshape(3, last - first, R, PW)

    def lead(q):
        for part in range(2):
            for i in range(2):
                y_direct(q, i, part).start()

    def gather_chunk(q):
        for i in range(2):
            y_direct(q, i, 0).wait_recv()
            y_forward(q, i).start()

    for k in range(8):
        for copy in loads(k):
            copy.start()
    base_load = pltpu.make_async_copy(base_hbm, base, ld.at[8, 0])

    barrier = pltpu.get_barrier_semaphore()
    peers = [at(dx, 0, core, 0) for dx, core in direct + two]
    peers += [at(0, dz, c, 0) for dz in (1, -1, 2, -2)] + [at(0, 0, c, dt) for dt in (1, -1)]
    for dev in peers:
        pl.semaphore_signal(barrier, inc=1, device_id=dev, device_id_type=MESH)

    for k in range(8):
        for copy in loads(k):
            copy.wait()
        cols = slice(k * PW, (k + 1) * PW)
        rows = a_v[cols, :].T
        own[:, :, :, cols] = rows.reshape(3, NQ, R, PW)
        solve_panel(k, 0, FIRST)
    base_load.start()
    pl.semaphore_wait(barrier, len(peers))
    lead(0)

    lane = lax.broadcasted_iota(jnp.int32, (8, 128), 1)
    seat_tile = jnp.full((8, 128), 36, jnp.int32)
    seat_slot = jnp.full((8, 128), -1, jnp.int32)
    for a in range(12):
        d = lax.rem(a // 3 - t + NY, NY)
        rel = jnp.where(d == 0, 0, jnp.where(d == 3, 1, jnp.where(d == 1, 2, 3)))
        for b in range(3):
            o = owner_s[b, 0, a]
            seat = ((o // 16) * 2 + lax.rem(o, 2)) * 8 + lax.rem(o // 2, 8)
            here = lane == seat
            seat_tile = jnp.where(here, (rel * 3 + a % 3) * 3 + b, seat_tile)
            seat_slot = jnp.where(here, slot_s[b, 0, a], seat_slot)
    seats_v[0] = seat_tile
    seats_v[1] = seat_slot
    to_scalar = pltpu.make_async_copy(seats_v, seats_s, ld.at[8, 1])
    to_scalar.start()
    to_scalar.wait()
    for j in range(64):
        pages[j // 8, j % 8] = jnp.full((8, 128), seats_s[1, 0, j], jnp.int32)
    for i in range(7):
        label_group(i).start()
    for k in range(8):
        solve_panel(k, FIRST, NQ)
        if k == 5:
            gather_chunk(0)
            lead(1)
    tiles[36] = jnp.zeros((R, PW), jnp.bfloat16)
    for zz in range(NZ):
        RL[zz, g_own] = pages[g_own, zz]
    base_load.wait()

    def tile_view(ref, *index):
        return lambda cols: ref[(*index, slice(None), cols)]

    def page_view(ref, *index):
        return lambda: ref[index]

    def tick(step, carry):
        def stage(lag, run):
            q = step - lag

            @pl.when(jnp.logical_and(q >= 0, q < NQ))
            def _():
                run(q)

        def finish(q):
            for d in range(2):
                z_copy(q, d, 4).wait_recv()
            rows = pl.ds(pl.multiple_of(q * R, R), R)

            def write(j, cols, value):
                out[j, rows, cols] = value.astype(jnp.bfloat16)

            combine(
                [lambda j, cols: base[j, rows, cols]]
                + [lambda j, cols, d=d: B4[d, q, j, :, cols] for d in range(2)],
                [(tile_view(RA, q, z, g), page_view(RL, z, g)) for g in range(8)],
                write,
            )

        def hop4(q):
            for d in range(2):
                sign = 1 - 2 * d
                z_copy(q, d, 3).wait_recv()

                @pl.when(q >= RING)
                def _(d=d):
                    z_copy(q - RING, d, 4).wait_send()

                def write(j, cols, value, d=d):
                    C4[d, ring(q), j, :, cols] = value.astype(jnp.bfloat16)

                combine(
                    [lambda j, cols, d=d: B3[d, q, j, :, cols]],
                    [(tile_view(RA, q, zat(sign), g), page_view(RL, zat(sign), g)) for g in range(8)],
                    write,
                )
                z_copy(q, d, 4).start()

        def hop3(q):
            for d in range(2):
                sign = 1 - 2 * d
                z_copy(q, d, 1).wait_recv()
                z_copy(q, d, 2).wait_recv()

                @pl.when(q >= RING)
                def _(d=d):
                    z_copy(q - RING, d, 3).wait_send()

                def write(j, cols, value, d=d):
                    C3[d, ring(q), j, :, cols] = value.astype(jnp.bfloat16)

                combine(
                    [],
                    [(tile_view(B2, d, q, i), page_view(L2, d, i)) for i in range(4)]
                    + [(tile_view(B2, d, q, 4 + i), page_view(L1, d, i)) for i in range(8)]
                    + [(tile_view(RA, q, zat(2 * sign), g), page_view(RL, zat(2 * sign), g)) for g in range(8)],
                    write,
                )
                z_copy(q, d, 3).start()

        def hop2(q):
            for d in range(2):
                z_copy(q, d, 0).wait_recv()
                z_copy(q, d, 1).start()
                z_copy(q, d, 2).start()

        def hop1(q):
            for i in range(1, 8):
                a_arrival(q, lax.rem(g_own + i, 8)).wait_recv()
            for d in range(2):
                z_copy(q, d, 0).start()

        def relay(q):
            for i in range(2):
                a_transit(q, i).wait_recv()
                a_forward(q, i).start()

        def form(q):
            for i in range(2):
                y_direct(q, i, 1).wait_recv()
                y_forward(q, i).wait_recv()
            left = jnp.concatenate(
                [own[:, q].reshape(3 * R, 2048), G[q].reshape(9 * R, 2048)], axis=0
            )
            for b in range(3):
                gram = dot_nt(left, own[b].reshape(PW, 2048))
                for p in range(12):
                    tiles[p * 3 + b] = (-gram[p * R : (p + 1) * R]).astype(jnp.bfloat16)
            for j in range(64):
                S[q, j // 8, j % 8] = tiles[seats_s[0, 0, j]]
            for i in range(2):
                a_transit(q, i).start()
            for i in range(5):
                a_direct(q, i).start()
            for zz in range(NZ):
                RA[q, zz, g_own] = S[q, g_own, zz]

        def labels_on():
            for i in range(1, 8):
                label_arrival(lax.rem(g_own + i, 8)).wait_recv()
            for d in range(2):
                for i in range(2):
                    label_z(d, i).start()

        def labels_in():
            for d in range(2):
                for i in range(2):
                    label_z(d, i).wait_recv()

        pl.when(step == 2)(labels_in)
        stage(1, relay)
        pl.when(step == 1)(labels_on)

        @pl.when(step + 1 < NQ)
        def _():
            gather_chunk(step + 1)

        @pl.when(step + 2 < NQ)
        def _():
            lead(step + 2)

        stage(2, hop2)
        stage(0, form)
        stage(1, hop1)
        stage(6, finish)
        stage(4, hop4)
        stage(2, hop3)
        return carry

    lax.fori_loop(0, NQ + 6, tick, 0)

    for i, whole in enumerate((G, G, B3)):
        rc(whole, whole, ss.at[i], ss.at[i], at(0, 0, 1 - c, 0)).wait_send()
    for q in range(NQ - RING, NQ):
        for d in range(2):
            for h in (3, 4):
                z_copy(q, d, h).wait_send()
    for i in range(7):
        label_group(i).wait_send()
    for d in range(2):
        for i in range(2):
            label_z(d, i).wait_send()


def shards(coupling, panel_inv, a_ib, owner, slot, base):
    vmem = pl.BlockSpec(memory_space=pltpu.VMEM)
    smem = pl.BlockSpec(memory_space=pltpu.SMEM)
    hbm = pl.BlockSpec(memory_space=pl.ANY)
    bf16, i32 = jnp.bfloat16, jnp.int32
    dma = pltpu.SemaphoreType.DMA
    result = pl.pallas_call(
        schur_kernel,
        out_shape=pltpu.VMEM((16, PW, PW), bf16),
        in_specs=[smem, smem, hbm, hbm, hbm, hbm],
        out_specs=vmem,
        scratch_shapes=[
            pltpu.VMEM((28, PW, PW), bf16),
            pltpu.VMEM((8, PW, PW), jnp.float32),
            pltpu.VMEM((2048, 768), bf16),
            pltpu.VMEM((16, PW, PW), bf16),
            pltpu.VMEM((3, NQ, R, 2048), bf16),
            pltpu.VMEM((2, 8, 128), i32),
            pltpu.SMEM((2, 8, 128), i32),
            pltpu.VMEM((8, 8, 8, 128), i32),
            pltpu.VMEM((NQ, 3, 3, R, 2048), bf16),
            pltpu.VMEM((NQ, 8, 8, R, PW), bf16),
            pltpu.VMEM((NQ, 8, 8, R, PW), bf16),
            pltpu.VMEM((NQ, 2, 8, R, PW), bf16),
            pltpu.VMEM((2, NQ, 4, R, PW), bf16),
            pltpu.VMEM((2, NQ, 12, R, PW), bf16),
            pltpu.VMEM((2, NQ, 16, R, PW), bf16),
            pltpu.VMEM((2, NQ, 16, R, PW), bf16),
            pltpu.VMEM((2, RING, 16, R, PW), bf16),
            pltpu.VMEM((2, RING, 16, R, PW), bf16),
            pltpu.VMEM((37, R, PW), bf16),
            pltpu.VMEM((8, 8, 8, 128), i32),
            pltpu.VMEM((2, 8, 8, 128), i32),
            pltpu.VMEM((2, 4, 8, 128), i32),
            dma((9, 3)),
            dma((3,)),
            dma((RING, 6)), dma((RING, 8)), dma((RING, 2)),
            dma((RING, 4)), dma((RING, 10)),
            dma((11,)), dma((8,)), dma((4,)),
        ],
        compiler_params=pltpu.CompilerParams(
            collective_id=0, has_side_effects=True, vmem_limit_bytes=VMEM_LIMIT
        ),
        name="schur",
    )(
        owner.transpose(2, 0, 1),
        slot.transpose(2, 0, 1),
        coupling[0],
        panel_inv[0],
        a_ib[0],
        base[0],
    )
    return result[None]


def solution(mesh):
    placed = (
        P("sub", None, None, None),
        P("sub", None, None, None),
        P("sub", None, "tile"),
        P("sub", None, "tile"),
        P("sub", None, "tile"),
        P("sub", "tile", None, None),
    )
    return jax.shard_map(
        shards, mesh=mesh, in_specs=placed, out_specs=P("sub", "tile", None, None), check_vma=False
    )
```

```python
import functools

import jax
import jax.numpy as jnp
from jax import lax
from jax.experimental import pallas as pl
from jax.experimental.pallas import tpu as pltpu
from jax.sharding import PartitionSpec as P

MESH = pl.DeviceIdType.MESH
NX, NZ, NC, NY = 4, 8, 2, 4
PW = 256
NQ = 16
R = PW // NQ
FIRST = 4
RING = 4
VMEM_LIMIT = 59 * 2**20
NT = (((1,), (1,)), ((), ()))


def dot_nt(left, right):
    return lax.dot_general(left, right, NT, preferred_element_type=jnp.float32)


def split_hi_lo(value):
    high = value.astype(jnp.bfloat16)
    low = (value - high.astype(jnp.float32)).astype(jnp.bfloat16)
    return high, low


def combine(dense, tiles, write):
    for half in range(2):
        cols = slice(half * 128, half * 128 + 128)
        acc = [None] * 16
        for view in dense:
            for j in range(16):
                x = view(j, cols).astype(jnp.float32)
                acc[j] = x if acc[j] is None else acc[j] + x
        for view, page in tiles:
            x = view(cols).astype(jnp.float32)
            lab = page()
            lab = jnp.concatenate([lab] * (R // 8), axis=0)
            for j in range(16):
                term = jnp.where(lab == j, x, 0.0)
                acc[j] = term if acc[j] is None else acc[j] + term
        for j in range(16):
            write(j, cols, acc[j])


def schur_kernel(
    owner_s, slot_s, c_hbm, inv_hbm, a_hbm, base_hbm, out,
    c_v, inv_v, a_v, base, own, seats_v, seats_s, pages,
    G, S, RA, T, B1, B2, B3, B4, C3, C4, tiles, RL, L1, L2,
    ld, ss, ry, ra, rt, sz, rz, sl, rl, rlz,
):
    s = lax.axis_index("sub")
    t = lax.axis_index("tile")
    x, z, c = s // 16, lax.rem(s // 2, NZ), lax.rem(s, 2)
    g_own = x * 2 + c

    def at(dx, dz, core, dt):
        xx = lax.rem(x + dx + NX, NX)
        zz = lax.rem(z + dz + NZ, NZ)
        return ((xx * NZ + zz) * NC + core, lax.rem(t + dt + NY, NY))

    def group(dx, core):
        return lax.rem(x + dx + NX, NX) * 2 + core

    def ring(q):
        return lax.rem(q, RING)

    def zat(dz):
        return lax.rem(z + dz + NZ, NZ)

    def rc(src, dst, ss, rs, dev):
        return pltpu.make_async_remote_copy(
            src_ref=src, dst_ref=dst, send_sem=ss, recv_sem=rs, device_id=dev, device_id_type=MESH
        )

    direct = [(1, 0), (1, 1), (-1, 0), (-1, 1), (0, 1 - c)]
    two = [(2, 0), (2, 1)]

    def y_direct(q, i, part):
        lanes = pl.ds(1024 * (i if part == 0 else 1 - i), 1024)
        return rc(
            own.at[:, q, :, lanes], G.at[q, i, :, :, lanes],
            ss.at[0], ry.at[ring(q), 2 * i + part], at(0, 0, c, (1, -1)[i]),
        )

    def y_forward(q, i):
        lanes = pl.ds(i * 1024, 1024)
        return rc(
            G.at[q, i, :, :, lanes], G.at[q, 2, :, :, lanes],
            ss.at[0], ry.at[ring(q), 4 + i], at(0, 0, c, (1, -1)[i]),
        )

    def a_direct(q, i):
        dx, core = direct[i]
        return rc(
            S.at[q, group(dx, core)], RA.at[q, :, g_own], ss.at[1], ra.at[ring(q), g_own], at(dx, 0, core, 0)
        )

    def a_transit(q, i):
        return rc(
            S.at[q, group(2, i)], T.at[q, i], ss.at[1], rt.at[ring(q), i], at((1, -1)[i], 0, c, 0)
        )

    def a_forward(q, i):
        src_g = group((-1, 1)[i], c)
        return rc(
            T.at[q, i], RA.at[q, :, src_g], ss.at[1], ra.at[ring(q), src_g], at((1, -1)[i], 0, i, 0)
        )

    def a_arrival(q, g):
        return rc(S.at[q, g], RA.at[q, :, g], ss.at[1], ra.at[ring(q), g], at(0, 0, 1 - c, 0))

    def z_copy(q, d, h):
        sign = 1 - 2 * d
        dev = at(0, sign, c, 0)
        send = ss.at[2] if h < 3 else sz.at[ring(q), d * 2 + h - 3]
        if h == 0:
            src, dst = RA.at[q, zat(4), pl.ds(4 * d, 4)], B1.at[d, q]
        elif h == 1:
            src, dst = B1.at[d, q], B2.at[d, q, pl.ds(0, 4)]
        elif h == 2:
            src, dst = RA.at[q, zat(3 * sign)], B2.at[d, q, pl.ds(4, 8)]
        elif h == 3:
            src, dst = C3.at[d, ring(q)], B3.at[d, q]
        else:
            src, dst = C4.at[d, ring(q)], B4.at[d, q]
        return rc(src, dst, send, rz.at[ring(q), d * 5 + h], dev)

    def label_group(i):
        dx, core = (direct + two)[i]
        return rc(pages.at[group(dx, core)], RL.at[:, g_own], sl.at[i], rl.at[g_own], at(dx, 0, core, 0))

    def label_arrival(g):
        return rc(pages.at[g], RL.at[:, g], sl.at[0], rl.at[g], at(0, 0, 1 - c, 0))

    def label_z(d, i):
        sign = 1 - 2 * d
        if i == 0:
            src, dst = RL.at[zat(3 * sign)], L1.at[d]
        else:
            src, dst = RL.at[zat(4), pl.ds(4 * d, 4)], L2.at[d]
        return rc(src, dst, sl.at[7 + 2 * d + i], rlz.at[2 * d + i], at(0, sign * (1 + i), c, 0))

    def loads(k):
        rows = pl.ds(k * PW, PW)
        copies = [
            pltpu.make_async_copy(a_hbm.at[rows], a_v.at[rows], ld.at[k, 0]),
            pltpu.make_async_copy(inv_hbm.at[k], inv_v.at[k], ld.at[k, 1]),
        ]
        if k:
            blocks = pl.ds(k * (k - 1) // 2, k)
            copies.append(pltpu.make_async_copy(c_hbm.at[blocks], c_v.at[blocks], ld.at[k, 2]))
        return copies

    def solve_panel(k, first, last):
        count = 3 * (last - first) * R
        cols = slice(k * PW, (k + 1) * PW)
        target = own[:, first:last, :, cols].reshape(count, PW).astype(jnp.float32)
        if k:
            start = k * (k - 1) // 2
            joined = jnp.concatenate([c_v[start + m] for m in range(k)], axis=1)
            target = target - dot_nt(own[:, first:last, :, : k * PW].reshape(count, k * PW), joined)
        t_hi, t_lo = split_hi_lo(target)
        i_hi, i_lo = split_hi_lo(inv_v[k])
        solved = dot_nt(
            jnp.concatenate([t_hi, t_hi, t_lo], axis=1), jnp.concatenate([i_hi, i_lo, i_hi], axis=1)
        )
        own[:, first:last, :, cols] = solved.astype(jnp.bfloat16).reshape(3, last - first, R, PW)

    def lead(q):
        for part in range(2):
            for i in range(2):
                y_direct(q, i, part).start()

    def gather_chunk(q):
        for i in range(2):
            y_direct(q, i, 0).wait_recv()
            y_forward(q, i).start()

    for k in range(8):
        for copy in loads(k):
            copy.start()
    base_load = pltpu.make_async_copy(base_hbm, base, ld.at[8, 0])

    barrier = pltpu.get_barrier_semaphore()
    peers = [at(dx, 0, core, 0) for dx, core in direct + two]
    peers += [at(0, dz, c, 0) for dz in (1, -1, 2, -2)] + [at(0, 0, c, dt) for dt in (1, -1)]
    for dev in peers:
        pl.semaphore_signal(barrier, inc=1, device_id=dev, device_id_type=MESH)

    for k in range(8):
        for copy in loads(k):
            copy.wait()
        cols = slice(k * PW, (k + 1) * PW)
        rows = a_v[cols, :].T
        own[:, :, :, cols] = rows.reshape(3, NQ, R, PW)
        solve_panel(k, 0, FIRST)
    base_load.start()
    pl.semaphore_wait(barrier, len(peers))
    lead(0)

    lane = lax.broadcasted_iota(jnp.int32, (8, 128), 1)
    seat_tile = jnp.full((8, 128), 36, jnp.int32)
    seat_slot = jnp.full((8, 128), -1, jnp.int32)
    for a in range(12):
        d = lax.rem(a // 3 - t + NY, NY)
        rel = jnp.where(d == 0, 0, jnp.where(d == 3, 1, jnp.where(d == 1, 2, 3)))
        for b in range(3):
            o = owner_s[b, 0, a]
            seat = ((o // 16) * 2 + lax.rem(o, 2)) * 8 + lax.rem(o // 2, 8)
            here = lane == seat
            seat_tile = jnp.where(here, (rel * 3 + a % 3) * 3 + b, seat_tile)
            seat_slot = jnp.where(here, slot_s[b, 0, a], seat_slot)
    seats_v[0] = seat_tile
    seats_v[1] = seat_slot
    to_scalar = pltpu.make_async_copy(seats_v, seats_s, ld.at[8, 1])
    to_scalar.start()
    to_scalar.wait()
    for j in range(64):
        pages[j // 8, j % 8] = jnp.full((8, 128), seats_s[1, 0, j], jnp.int32)
    for i in range(7):
        label_group(i).start()
    for k in range(8):
        solve_panel(k, FIRST, NQ)
        if k == 5:
            gather_chunk(0)
            lead(1)
    tiles[36] = jnp.zeros((R, PW), jnp.bfloat16)
    for zz in range(NZ):
        RL[zz, g_own] = pages[g_own, zz]
    base_load.wait()

    def tile_view(ref, *index):
        return lambda cols: ref[(*index, slice(None), cols)]

    def page_view(ref, *index):
        return lambda: ref[index]

    def tick(step, carry):
        def stage(lag, run):
            q = step - lag

            @pl.when(jnp.logical_and(q >= 0, q < NQ))
            def _():
                run(q)

        def finish(q):
            for d in range(2):
                z_copy(q, d, 4).wait_recv()
            rows = pl.ds(pl.multiple_of(q * R, R), R)

            def write(j, cols, value):
                out[j, rows, cols] = value.astype(jnp.bfloat16)

            combine(
                [lambda j, cols: base[j, rows, cols]]
                + [lambda j, cols, d=d: B4[d, q, j, :, cols] for d in range(2)],
                [(tile_view(RA, q, z, g), page_view(RL, z, g)) for g in range(8)],
                write,
            )

        def hop4(q):
            for d in range(2):
                sign = 1 - 2 * d
                z_copy(q, d, 3).wait_recv()

                @pl.when(q >= RING)
                def _(d=d):
                    z_copy(q - RING, d, 4).wait_send()

                def write(j, cols, value, d=d):
                    C4[d, ring(q), j, :, cols] = value.astype(jnp.bfloat16)

                combine(
                    [lambda j, cols, d=d: B3[d, q, j, :, cols]],
                    [(tile_view(RA, q, zat(sign), g), page_view(RL, zat(sign), g)) for g in range(8)],
                    write,
                )
                z_copy(q, d, 4).start()

        def hop3(q):
            for d in range(2):
                sign = 1 - 2 * d
                z_copy(q, d, 1).wait_recv()
                z_copy(q, d, 2).wait_recv()

                @pl.when(q >= RING)
                def _(d=d):
                    z_copy(q - RING, d, 3).wait_send()

                def write(j, cols, value, d=d):
                    C3[d, ring(q), j, :, cols] = value.astype(jnp.bfloat16)

                combine(
                    [],
                    [(tile_view(B2, d, q, i), page_view(L2, d, i)) for i in range(4)]
                    + [(tile_view(B2, d, q, 4 + i), page_view(L1, d, i)) for i in range(8)]
                    + [(tile_view(RA, q, zat(2 * sign), g), page_view(RL, zat(2 * sign), g)) for g in range(8)],
                    write,
                )
                z_copy(q, d, 3).start()

        def hop2(q):
            for d in range(2):
                z_copy(q, d, 0).wait_recv()
                z_copy(q, d, 1).start()
                z_copy(q, d, 2).start()

        def hop1(q):
            for i in range(1, 8):
                a_arrival(q, lax.rem(g_own + i, 8)).wait_recv()
            for d in range(2):
                z_copy(q, d, 0).start()

        def relay(q):
            for i in range(2):
                a_transit(q, i).wait_recv()
                a_forward(q, i).start()

        def form(q):
            for i in range(2):
                y_direct(q, i, 1).wait_recv()
                y_forward(q, i).wait_recv()
            left = jnp.concatenate(
                [own[:, q].reshape(3 * R, 2048), G[q].reshape(9 * R, 2048)], axis=0
            )
            for b in range(3):
                gram = dot_nt(left, own[b].reshape(PW, 2048))
                for p in range(12):
                    tiles[p * 3 + b] = (-gram[p * R : (p + 1) * R]).astype(jnp.bfloat16)
            def pack(dst, g):
                for zz in range(NZ):
                    dst(zz)[...] = tiles[seats_s[0, 0, g * NZ + zz]]

            for i in range(2):
                far = group(2, i)
                pack(lambda zz, far=far: S.at[q, far, zz], far)
                a_transit(q, i).start()
            for i in range(5):
                near = group(*direct[i])
                pack(lambda zz, near=near: S.at[q, near, zz], near)
                a_direct(q, i).start()
            pack(lambda zz: RA.at[q, zz, g_own], g_own)

        def labels_on():
            for i in range(1, 8):
                label_arrival(lax.rem(g_own + i, 8)).wait_recv()
            for d in range(2):
                for i in range(2):
                    label_z(d, i).start()

        def labels_in():
            for d in range(2):
                for i in range(2):
                    label_z(d, i).wait_recv()

        pl.when(step == 2)(labels_in)
        stage(1, relay)
        pl.when(step == 1)(labels_on)

        @pl.when(step + 1 < NQ)
        def _():
            gather_chunk(step + 1)

        @pl.when(step + 2 < NQ)
        def _():
            lead(step + 2)

        stage(2, hop2)
        stage(0, form)
        stage(1, hop1)
        stage(6, finish)
        stage(4, hop4)
        stage(2, hop3)
        return carry

    lax.fori_loop(0, NQ + 6, tick, 0)

    for i, whole in enumerate((G, G, B3)):
        rc(whole, whole, ss.at[i], ss.at[i], at(0, 0, 1 - c, 0)).wait_send()
    for q in range(NQ - RING, NQ):
        for d in range(2):
            for h in (3, 4):
                z_copy(q, d, h).wait_send()
    for i in range(7):
        label_group(i).wait_send()
    for d in range(2):
        for i in range(2):
            label_z(d, i).wait_send()


def shards(coupling, panel_inv, a_ib, owner, slot, base):
    vmem = pl.BlockSpec(memory_space=pltpu.VMEM)
    smem = pl.BlockSpec(memory_space=pltpu.SMEM)
    hbm = pl.BlockSpec(memory_space=pl.ANY)
    bf16, i32 = jnp.bfloat16, jnp.int32
    dma = pltpu.SemaphoreType.DMA
    result = pl.pallas_call(
        schur_kernel,
        out_shape=pltpu.VMEM((16, PW, PW), bf16),
        in_specs=[smem, smem, hbm, hbm, hbm, hbm],
        out_specs=vmem,
        scratch_shapes=[
            pltpu.VMEM((28, PW, PW), bf16),
            pltpu.VMEM((8, PW, PW), jnp.float32),
            pltpu.VMEM((2048, 768), bf16),
            pltpu.VMEM((16, PW, PW), bf16),
            pltpu.VMEM((3, NQ, R, 2048), bf16),
            pltpu.VMEM((2, 8, 128), i32),
            pltpu.SMEM((2, 8, 128), i32),
            pltpu.VMEM((8, 8, 8, 128), i32),
            pltpu.VMEM((NQ, 3, 3, R, 2048), bf16),
            pltpu.VMEM((NQ, 8, 8, R, PW), bf16),
            pltpu.VMEM((NQ, 8, 8, R, PW), bf16),
            pltpu.VMEM((NQ, 2, 8, R, PW), bf16),
            pltpu.VMEM((2, NQ, 4, R, PW), bf16),
            pltpu.VMEM((2, NQ, 12, R, PW), bf16),
            pltpu.VMEM((2, NQ, 16, R, PW), bf16),
            pltpu.VMEM((2, NQ, 16, R, PW), bf16),
            pltpu.VMEM((2, RING, 16, R, PW), bf16),
            pltpu.VMEM((2, RING, 16, R, PW), bf16),
            pltpu.VMEM((37, R, PW), bf16),
            pltpu.VMEM((8, 8, 8, 128), i32),
            pltpu.VMEM((2, 8, 8, 128), i32),
            pltpu.VMEM((2, 4, 8, 128), i32),
            dma((9, 3)),
            dma((3,)),
            dma((RING, 6)), dma((RING, 8)), dma((RING, 2)),
            dma((RING, 4)), dma((RING, 10)),
            dma((11,)), dma((8,)), dma((4,)),
        ],
        compiler_params=pltpu.CompilerParams(
            collective_id=0, has_side_effects=True, vmem_limit_bytes=VMEM_LIMIT
        ),
        name="schur",
    )(
        owner.transpose(2, 0, 1),
        slot.transpose(2, 0, 1),
        coupling[0],
        panel_inv[0],
        a_ib[0],
        base[0],
    )
    return result[None]


def solution(mesh):
    placed = (
        P("sub", None, None, None),
        P("sub", None, None, None),
        P("sub", None, "tile"),
        P("sub", None, "tile"),
        P("sub", None, "tile"),
        P("sub", "tile", None, None),
    )
    return jax.shard_map(
        shards, mesh=mesh, in_specs=placed, out_specs=P("sub", "tile", None, None), check_vma=False
    )
```
